256 devices in a mesh: ctx: 8 (over z), exp: 32 (over x, y, core).
Axes of the slice: x: 4, y: 4, z: 8, core: 2. Of those that a mesh axis runs over, the one named last changes fastest.
Arguments:
- q_latent: bfloat16 [128, 128, 512], P('exp'), may hold values from -7 to 7
- q_rope: bfloat16 [128, 64, 128], P('exp'), may hold values from -84 to 84
- cache_latent: bfloat16 [128, 4096, 512], P('exp', 'ctx'), may hold values from -6 to 6
- cache_rope: bfloat16 [128, 64, 4096], P('exp', None, 'ctx'), may hold values from -6 to 6
- lengths: int32 [128], P('exp'), may hold values from 1024 to 4096
- w_attn_out: bfloat16 [128, 512, 7168], P('ctx', None, 'exp'), may hold values from -0.1875 to 0.1875
- hidden_in: bfloat16 [128, 7168], P(None, 'exp'), may hold values from -6 to 6
- norm_gain: bfloat16 [7168], replicated, may hold values from 0.5 to 8
- w_gate: bfloat16 [32, 7168, 1024], P('exp', None, 'ctx'), may hold values from -0.0625 to 0.0625
- w_up: bfloat16 [32, 7168, 1024], P('exp', None, 'ctx'), may hold values from -0.0625 to 0.0625
- w_down: bfloat16 [32, 1024, 7168], P('exp', 'ctx'), may hold values from -0.1875 to 0.1875
- expert_ids: int32 [128, 8], replicated, may hold values from 0 to 31, all different within a row; in each aligned block of 128 rows (0 to 127, 128 to 255, ...) at most 64 rows name the same one
- gate_weights: float32 [128, 8], replicated, may hold values from 0.1 to 1
Outputs:
- layer_out: bfloat16 [128, 7168], P('exp', 'ctx')
The draws below stay inside these ranges and needn't reach their ends.
Inputs may be any that keep to these rules, and one draw needn't show every extreme that they name: `expert_ids`: each row names 8 different experts; over all 128 rows no expert is named more than 64 times, a bound that some block reaches.
All inputs are finite; a program needn't handle non-finite values.
Results may differ from the reference program's by a relative error of at most 0.008.
Values may be sent and summed in bfloat16 or wider, within the bound.
A program may use at most 64 MiB of HBM per device.

```python
import math
import jax
import jax.numpy as jnp
import numpy as np
from jax import lax

D = 7168
H = 128
DL = 512
DR = 64
FF = 1024
TOPK = 8
CTX_DEV = 512
ROWS = 128
CTX = 4096
EXPERTS = 32
E_CAP = 64
N_CTX = 8
N_EXP = 32


def draw_cache_rope(key, part):
    drawn = jnp.clip(jax.random.normal(jax.random.fold_in(key, 7101), (ROWS, DR, CTX), jnp.float32), -6.0, 6.0)
    return drawn.astype(jnp.bfloat16)


def draw_q_rope(key, part):
    drawn = jnp.clip(jax.random.normal(jax.random.fold_in(key, 7203), (ROWS, DR, H), jnp.float32), -6.0, 6.0)
    return drawn.astype(jnp.bfloat16)


def draw_q_latent(key, part):
    drawn = jnp.clip(jax.random.normal(jax.random.fold_in(key, 7302), (ROWS, H, DL), jnp.float32), -6.0, 6.0)
    return drawn.astype(jnp.bfloat16)


def draw_norm_gain(key, part):
    base = 1.0 + 0.18 * jax.random.uniform(jax.random.fold_in(key, 7401), (D,), jnp.float32, -1.0, 1.0)
    block_width = D // N_EXP
    heavy_block = jax.random.randint(jax.random.fold_in(key, 7402), (), 0, N_EXP)
    in_block = jnp.arange(D, dtype=jnp.int32) // block_width == heavy_block
    heavy = jax.random.uniform(jax.random.fold_in(key, 7403), (D,), jnp.float32, 4.0, 6.0)
    return jnp.where(in_block, heavy, base).astype(jnp.bfloat16)


def plant(drawn, stream_key, low, top_value):
    longest = drawn.shape.index(max(drawn.shape))
    spots = []
    for shift in (0, 1):
        where = [jax.random.randint(jax.random.fold_in(stream_key, axis), (), 0, length) for axis, length in enumerate(drawn.shape)]
        where[longest] = (where[longest] + shift) % drawn.shape[longest]
        spots.append(tuple(where))
    return drawn.at[spots[0]].set(low).at[spots[1]].set(top_value)


def block_levels(own_key, extent, cuts, smallest, largest):
    def one(axis_at, blocks):
        heights = jax.random.uniform(jax.random.fold_in(jax.random.fold_in(own_key, 6), axis_at), (blocks,), jnp.float32, smallest / len(cuts), largest / len(cuts))
        return jnp.repeat(jnp.exp(heights), extent[axis_at] // blocks).reshape((-1,) + (1,) * (len(extent) - axis_at - 1))

    level = one(*cuts[0])
    for cut in cuts[1:]:
        level = level * one(*cut)
    return level


def assign_block(own_key, own, number, rows, count, top, most, skew):
    order = jax.random.permutation(own_key, count)
    heavy_load, common = shares(count, rows * top, most, skew, True), shares(count, rows * top, most, skew, False)
    places = jnp.arange(count)

    def named(sizes, offset_by):
        used = int((sizes > 0).sum())
        fixed = max(1, used // 4)
        shifted = fixed + (places - fixed + offset_by * (used - fixed)) % max(1, count - fixed)
        return jnp.zeros((count,), jnp.int32).at[order[jnp.where(places < fixed, places, shifted)]].set(jnp.asarray(sizes, jnp.int32))

    sizes = jnp.where(number % 4 == 0, named(heavy_load, number // 4), named(common, number - number // 4 - 1))
    mixed = jax.random.permutation(jax.random.fold_in(own, 3), count)
    giver, receiver = mixed[0:count // 2 * 2:2], mixed[1:count // 2 * 2:2]
    margin = jnp.minimum(sizes[giver] - 1, most - sizes[receiver]) // 2
    margin = jnp.where((giver == order[0]) | (receiver == order[0]) | (sizes[receiver] == 0), 0, jnp.maximum(margin, 0))
    shifted = jax.random.randint(jax.random.fold_in(own, 4), (count // 2,), 0, 1 << 20) % (margin + 1)
    sizes = sizes.at[giver].add(-shifted).at[receiver].add(shifted)
    members = jnp.searchsorted(jnp.cumsum(sizes), jnp.arange(rows * top), side="right").astype(jnp.int32)
    listing = members.reshape(top, rows).T
    listing = listing[jax.random.permutation(jax.random.fold_in(own, 1), rows)]
    offset_by = jax.random.randint(jax.random.fold_in(own, 2), (rows, 1), 0, top)
    return jnp.take_along_axis(listing, (jnp.arange(top)[None, :] + offset_by) % top, axis=1)


def shares(amount, total, most, lean, full):
    weights = [(1 << 20) // math.isqrt(grade ** lean) + 1 for grade in range(1, amount + 1)]
    largest = most if full else min(most, max(-(-total // amount), total * weights[0] // sum(weights)))
    least = 1 if total - largest >= amount - 1 else 0
    counts, surplus = [largest] + [least] * (amount - 1), total - largest - least * (amount - 1)
    while surplus > 0:
        candidates = [i for i in range(1, amount) if counts[i] < largest] or [i for i in range(1, amount) if counts[i] < most]
        whole, left = sum([weights[i] for i in candidates]), surplus
        for i in candidates:
            addition = min(most - counts[i], max(1, left * weights[i] // whole), surplus)
            counts[i] = counts[i] + addition
            surplus = surplus - addition
    return np.array(counts)


def scatter_about(stream_key, dims, deviation, most, cuts=(), kind=jnp.bfloat16):
    loudness = block_levels(stream_key, dims, cuts, -0.22, 0.18) if cuts else 1.0
    values = jax.random.normal(stream_key, dims, jnp.float32) * deviation * loudness
    return jnp.minimum(jnp.maximum(values, -most), most).astype(kind)


def setup_inputs(seed: int = 0) -> dict:
    streams_of = jax.random.split(jax.random.key(seed), 14)
    q_latent = draw_q_latent(jax.random.fold_in(streams_of[13], 71), 0)
    q_rope = draw_q_rope(jax.random.fold_in(streams_of[13], 71), 0)
    cache_latent = scatter_about(streams_of[2], (ROWS, CTX, DL), 1.0, 6.0, ((0, 32), (1, 8)))
    cache_rope = draw_cache_rope(jax.random.fold_in(streams_of[13], 71), 0)
    lengths = plant(jax.random.randint(streams_of[4], (ROWS,), CTX // 4, CTX + 1), jax.random.fold_in(streams_of[4], 1), CTX // 4, CTX).astype(jnp.int32)
    w_attn_out = scatter_about(streams_of[5], (H, DL, D), (H * DL // 64) ** -0.5, 0.1875, ((0, 8), (2, 32)))
    hidden_in = scatter_about(streams_of[6], (ROWS, D), 1.0, 6.0, ((1, 32),))
    norm_gain = draw_norm_gain(jax.random.fold_in(streams_of[13], 71), 0)
    w_gate = scatter_about(streams_of[8], (EXPERTS, D, FF), D ** -0.5, 0.0625, ((0, 32), (2, 8)))
    w_up = scatter_about(streams_of[9], (EXPERTS, D, FF), D ** -0.5, 0.0625, ((0, 32), (2, 8)))
    w_down = scatter_about(streams_of[10], (EXPERTS, FF, D), FF ** -0.5, 0.1875, ((0, 32), (1, 8)))
    expert_ids_keys = jax.random.split(jax.random.fold_in(streams_of[11], 1), ROWS // ROWS)
    expert_ids_turns = jax.random.permutation(jax.random.fold_in(streams_of[11], 3), ROWS // ROWS)
    expert_ids = jax.vmap(lambda own, number: assign_block(jax.random.fold_in(streams_of[11], 2), own, number, ROWS, EXPERTS, TOPK, E_CAP, 2))(expert_ids_keys, expert_ids_turns).reshape((ROWS, TOPK))
    gate_weights = jnp.clip(jax.random.uniform(streams_of[12], (ROWS, TOPK), jnp.float32, 0.1, 1.0), 0.1, 1.0)
    return {"q_latent": q_latent, "q_rope": q_rope, "cache_latent": cache_latent, "cache_rope": cache_rope, "lengths": lengths, "w_attn_out": w_attn_out, "hidden_in": hidden_in, "norm_gain": norm_gain, "w_gate": w_gate, "w_up": w_up, "w_down": w_down, "expert_ids": expert_ids, "gate_weights": gate_weights}


SOFTMAX_SCALE = 192.0 ** (-0.5)
MASKED = -1e+30
EPSILON = 1e-06

def slot_tables(expert_ids, gate_weights, experts, capacity):
    row_count, top_count = expert_ids.shape
    flat_ids = expert_ids.reshape(-1)
    one_hot = (flat_ids[:, None] == jnp.arange(experts, dtype=jnp.int32)[None, :]).astype(jnp.int32)
    before = jnp.cumsum(one_hot, axis=0) - one_hot
    slot_index = lax.optimization_barrier(jnp.sum(before * one_hot, axis=1))
    target = (flat_ids * capacity + slot_index).astype(jnp.int32)
    owner_row = (jnp.arange(row_count * top_count, dtype=jnp.int32) // top_count).astype(jnp.int32)
    slot_row = jnp.full((experts * capacity,), row_count, jnp.int32).at[target].set(owner_row)
    slot_gate = jnp.zeros((experts * capacity,), jnp.float32).at[target].set(gate_weights.reshape(-1))
    return (slot_row, slot_gate)

def attend_row(row_inputs):
    query_latent, query_rope, keys_latent, keys_rope, length = row_inputs
    scores = jnp.dot(query_latent, keys_latent.T, preferred_element_type=jnp.float32)
    scores = (scores + jnp.dot(query_rope.T, keys_rope, preferred_element_type=jnp.float32)) * SOFTMAX_SCALE
    visible = jnp.arange(CTX, dtype=jnp.int32) < length
    scores = jnp.where(visible[None, :], scores, MASKED)
    blocked = scores.reshape(H, N_CTX, CTX_DEV)
    seen_mask = visible.reshape(1, N_CTX, CTX_DEV)
    block_max = lax.optimization_barrier(jnp.max(blocked, axis=2))
    weights = jnp.where(seen_mask, jnp.exp(blocked - block_max[..., None]), 0.0)
    block_total = lax.optimization_barrier(jnp.sum(weights, axis=2))
    rounded = lax.optimization_barrier(weights.astype(jnp.bfloat16)).astype(jnp.float32)
    values = keys_latent.astype(jnp.float32).reshape(N_CTX, CTX_DEV, DL)
    block_value = jnp.einsum('hbp,bpl->hbl', rounded, values, precision=lax.Precision.HIGHEST)
    joint_max = lax.optimization_barrier(jnp.max(block_max, axis=1))
    rescale = jnp.exp(block_max - joint_max[:, None])
    grand_total = lax.optimization_barrier(jnp.sum(block_total * rescale, axis=1))
    grand_value = lax.optimization_barrier(jnp.sum(block_value * rescale[..., None], axis=1))
    return (grand_value / grand_total[:, None]).astype(jnp.bfloat16)

def reference(q_latent, q_rope, cache_latent, cache_rope, lengths, w_attn_out, hidden_in, norm_gain, w_gate, w_up, w_down, expert_ids, gate_weights):
    attended = lax.map(attend_row, (q_latent, q_rope, cache_latent, cache_rope, lengths))
    projected = jnp.dot(attended.reshape(ROWS, H * DL), w_attn_out.reshape(H * DL, D), preferred_element_type=jnp.float32)
    hidden_state = hidden_in.astype(jnp.float32) + projected
    slot_row, slot_gate = slot_tables(expert_ids, gate_weights, EXPERTS, E_CAP)
    rounded = lax.optimization_barrier(hidden_state.astype(jnp.bfloat16))
    padded = jnp.concatenate([rounded, jnp.zeros((1, D), jnp.bfloat16)], axis=0)

    def run_expert(expert_inputs):
        rows_here, gate_matrix, up_matrix, down_matrix = expert_inputs
        arriving = padded[rows_here]
        values = arriving.astype(jnp.float32)
        mean_square = lax.optimization_barrier(jnp.mean(values * values, axis=1, keepdims=True))
        normed = (values * lax.rsqrt(mean_square + EPSILON) * norm_gain.astype(jnp.float32)).astype(jnp.bfloat16)
        gate_part = jnp.dot(normed, gate_matrix, preferred_element_type=jnp.float32)
        up_part = jnp.dot(normed, up_matrix, preferred_element_type=jnp.float32)
        active = (jax.nn.silu(gate_part) * up_part).astype(jnp.bfloat16)
        return jnp.dot(active, down_matrix, preferred_element_type=jnp.float32)
    expert_out = lax.map(run_expert, (slot_row.reshape(EXPERTS, E_CAP), w_gate, w_up, w_down))
    weighted = expert_out.reshape(EXPERTS * E_CAP, D) * slot_gate[:, None]
    mixture = jax.ops.segment_sum(weighted, slot_row, num_segments=ROWS)
    return (hidden_state + mixture).astype(jnp.bfloat16)
```

```python
import functools

import jax
import jax.numpy as jnp
from jax import lax
from jax.experimental import pallas as pl
from jax.experimental.pallas import tpu as pltpu
from jax.sharding import PartitionSpec as P

SCALE = 192.0 ** (-0.5)
MASKED = -1e30
EPSILON = 1e-06
MESH = pl.DeviceIdType.MESH
BF = jnp.bfloat16
F32 = jnp.float32
NZ, NX, NY = 8, 4, 4
HALF = 3584
PART = 1792
TOP = pl.ds(0, PART)
BOT = pl.ds(PART, PART)


def dot(a, b, dims=(((1,), (0,)), ((), ()))):
    return lax.dot_general(a, b, dims, preferred_element_type=F32)


def kernel(
    q_hbm, qr_hbm, kc_hbm, kr_hbm, len_ref, wo_hbm, hid_hbm, gain_hbm, wg_hbm, wu_hbm, wd_hbm,
    ids_hbm, gw_hbm, out_ref,
    qv, qrv, kcv, krv, wov, hidv, gainv, wguv, wdv, idsv, gwv,
    vb, st_s, st_r, br, alv, gbuf, gf, ef, es, er, fg, gds, gsel, actf, actp,
    p1, m1, r1, p2, m2, r2, z3s, z3r,
    lsem, psend, precv, bsend, brecv, gsend, grecv, esend, erecv, fsend, frecv,
    hsend, hrecv, ssend, srecv, ksend, krecv, zsend, zrecv,
):
    z = lax.axis_index("ctx")
    e = lax.axis_index("exp")
    core = lax.rem(e, 2)
    p = lax.div(e, 2)
    y = lax.rem(p, NY)
    x = lax.div(p, NY)
    zq, zk = lax.div(z, 2), lax.rem(z, 2)

    def dev(dz=0, dx=0, dy=0, other=False):
        c = (1 - core) if other else core
        xx, yy = lax.rem(x + dx, NX), lax.rem(y + dy, NY)
        return {"ctx": lax.rem(z + dz, NZ), "exp": (xx * NY + yy) * 2 + c}

    barrier = pltpu.get_barrier_semaphore()
    peers = [dev(dz=d) for d in range(1, NZ)]
    peers += [dev(dx=1), dev(dx=3), dev(dy=1), dev(dy=3), dev(other=True)]
    for peer in peers:
        pl.semaphore_signal(barrier, inc=1, device_id=peer, device_id_type=MESH)

    def load(src, dst, k):
        return pltpu.make_async_copy(src, dst, lsem.at[k])

    row_loads = []
    for r in range(4):
        row_loads.append([
            load(q_hbm.at[r], qv.at[r], 4 * r),
            load(kc_hbm.at[r], kcv.at[r], 4 * r + 1),
            load(qr_hbm.at[r], qrv.at[r], 4 * r + 2),
            load(kr_hbm.at[r], krv.at[r], 4 * r + 3),
        ])
        for c in row_loads[r]:
            c.start()
    own = pl.ds(pl.multiple_of(core * 128, 128), 128)
    small_loads = [
        load(ids_hbm, idsv, 16),
        load(gw_hbm, gwv, 17),
        load(gain_hbm, gainv, 18),
        load(hid_hbm, hidv.at[core], 19),
    ]
    big_loads = [
        load(wo_hbm, wov.at[core], 20),
        load(wg_hbm, wguv.at[core, :, pl.ds(0, 224), pl.ds(0, 128)], 21),
        load(wu_hbm, wguv.at[core, :, pl.ds(0, 224), pl.ds(128, 128)], 22),
        load(wd_hbm, wdv.at[own], 23),
    ]
    for c in small_loads + big_loads:
        c.start()
    wguv[:, :, 224:256, :] = jnp.zeros((2, 32, 32, 256), BF)

    pl.semaphore_wait(barrier, len(peers))

    def swap(src, dst, k):
        return pltpu.make_async_remote_copy(
            src_ref=src, dst_ref=dst, send_sem=psend.at[k], recv_sem=precv.at[k],
            device_id=dev(other=True), device_id_type=MESH,
        )

    swaps = [
        swap(hid_hbm, hidv.at[core], 0),
        swap(wo_hbm, wov.at[core], 1),
        swap(wg_hbm, wguv.at[core, :, pl.ds(0, 224), pl.ds(0, 128)], 2),
        swap(wu_hbm, wguv.at[core, :, pl.ds(0, 224), pl.ds(128, 128)], 3),
        swap(wd_hbm, wdv.at[own], 4),
    ]
    for c in swaps:
        c.start()

    def remote(src, dst, ss, rs, device):
        return pltpu.make_async_remote_copy(
            src_ref=src, dst_ref=dst, send_sem=ss, recv_sem=rs,
            device_id=device, device_id_type=MESH,
        )

    def heads_of(zz):
        return pl.ds(pl.multiple_of(zz * 16, 16), 16)

    def value_copy(r, d):
        zz = lax.rem(z + d, NZ)
        return remote(
            vb.at[r, heads_of(zz)], br.at[z, r], bsend.at[r, d - 1], brecv.at[r, d - 1],
            dev(dz=d),
        )

    def stat_copy(d):
        return remote(st_s, st_r.at[z], bsend.at[4, d - 1], brecv.at[4, d - 1], dev(dz=d))

    lane = lax.broadcasted_iota(jnp.int32, (128, 128), 1)
    position = z * 512 + lax.broadcasted_iota(jnp.int32, (128, 512), 1)
    stats = jnp.zeros((128, 128), F32)
    for r in range(4):
        for c in row_loads[r]:
            c.wait()
        keys = kcv[r]
        scores = dot(qv[r], keys, (((1,), (1,)), ((), ())))
        scores = (scores + dot(qrv[r], krv[r], (((0,), (0,)), ((), ())))) * SCALE
        visible = position < len_ref[r]
        scores = jnp.where(visible, scores, MASKED)
        top = jnp.max(scores, axis=1, keepdims=True)
        weights = jnp.where(visible, jnp.exp(scores - top), 0.0)
        total = jnp.sum(weights, axis=1, keepdims=True)
        value = dot(weights.astype(BF), keys)
        held = jnp.maximum(total, 1e-30)
        vb[r] = (value / held).astype(BF)
        lse = jnp.where(total > 0.0, top + jnp.log(held), MASKED)
        stats = jnp.where(lane == r, lse, stats)
        if r == 3:
            st_s[...] = jnp.transpose(stats)[0:8]
            for d in range(1, NZ):
                stat_copy(d).start()
        for d in range(1, NZ):
            value_copy(r, d).start()
        br[z, r] = vb[r, heads_of(z)]
    st_r[z] = st_s[...]

    for c in small_loads:
        c.wait()
    for k in range(2):
        named = jnp.where(idsv[...] == 2 * p + k, gwv[...], 0.0)
        gds[:, 128 * k:128 * k + 128] = jnp.broadcast_to(
            jnp.sum(named, axis=1, keepdims=True), (128, 128)
        )
    for i in range(16):
        gsel[4 * i:4 * i + 4, :] = jnp.where(
            core == 0, gds[8 * i:8 * i + 4, :], gds[8 * i + 4:8 * i + 8, :]
        )

    for d in range(1, NZ):
        stat_copy(d).wait_recv()
    s = st_r[...]
    a = jnp.exp(s - jnp.max(s, axis=0, keepdims=True))
    a = a / jnp.sum(a, axis=0, keepdims=True)
    a = jnp.concatenate([a.reshape(64, 128), jnp.zeros((64, 128), F32)], axis=0)
    alv[...] = jnp.transpose(a)
    mine = alv[heads_of(z), :]
    for r in range(4):
        for d in range(1, NZ):
            value_copy(r, d).wait_recv()
        acc = jnp.zeros((16, 512), F32)
        for b in range(NZ):
            acc = acc + mine[:, 8 * b + r:8 * b + r + 1] * br[b, r].astype(F32)
        gbuf[x, y, r] = acc.astype(BF)

    def gatherer(buf, send, recv):
        def region(h, i1, i2, first, count):
            i1, i2 = lax.rem(i1, 4), lax.rem(i2, 4)
            xx, yy = (i1, i2) if h == 0 else (i2, i1)
            return buf.at[xx, yy, pl.ds(2 * h + first, count)]

        def copy(h, j, c):
            me1, me2 = (x, y) if h == 0 else (y, x)
            step = 1 if c in (0, 2) else 3
            first, count = {0: (0, 2), 1: (0, 2), 2: (0, 1), 3: (1, 1)}[c]
            shift = {0: 0, 1: 0, 2: 3, 3: 1}[c]
            if j == 4:
                ref = region(h, me1 + shift, me2, first, count)
                along_x = h == 0
            else:
                column = {0: 0, 1: 3, 2: 1, 3: 2}[j]
                ref = region(h, me1 + column, me2 + shift, first, count)
                along_x = h == 1
            target = dev(dx=step) if along_x else dev(dy=step)
            return remote(ref, ref, send.at[h, j, c], recv.at[h, j, c], target)

        for h in range(2):
            copy(h, 4, 0).start()
            copy(h, 4, 1).start()
        for h in range(2):
            copy(h, 0, 0).start()
            copy(h, 0, 1).start()
        for h in range(2):
            for c in range(2):
                copy(h, 4, c).wait_recv()
                copy(h, 4, c + 2).start()
                copy(h, 1 + c, 0).start()
                copy(h, 1 + c, 1).start()
        for j in range(3):
            for h in range(2):
                if j == 1:
                    copy(h, 4, 2).wait_recv()
                    copy(h, 4, 3).wait_recv()
                    copy(h, 3, 0).start()
                    copy(h, 3, 1).start()
                for c in range(2):
                    copy(h, j, c).wait_recv()
                    copy(h, j, c + 2).start()
        for h in range(2):
            for c in range(2):
                copy(h, 3, c).wait_recv()
                copy(h, 3, c + 2).start()
        for j in range(4):
            for h in range(2):
                copy(h, j, 2).wait_recv()
                copy(h, j, 3).wait_recv()
        return [copy(h, j, c) for h in range(2) for j in range(5) for c in range(4)]

    drains = [value_copy(r, d) for r in range(4) for d in range(1, NZ)]
    drains += [stat_copy(d) for d in range(1, NZ)]
    drains += gatherer(gbuf, gsend, grecv)

    for i in range(NX):
        rows = gbuf[i].reshape(256, 512).astype(F32)
        for t in range(4):
            gf[t, pl.ds(256 * i, 256), :] = rows[:, 128 * t:128 * t + 128]
    big_loads[0].wait()
    swaps[1].wait()

    def head(h, accs):
        lhs = jnp.concatenate(
            [gf[t, pl.ds(h, 64, stride=16), :] for t in range(4)], axis=1
        ).astype(BF)
        return (accs[0] + dot(lhs, wov[0, h]), accs[1] + dot(lhs, wov[1, h]))

    accs = lax.fori_loop(0, 16, head, (jnp.zeros((64, 224), F32), jnp.zeros((64, 224), F32)))
    for k in range(2):
        es[k] = jnp.concatenate([accs[k], jnp.zeros((64, 32), F32)], axis=1).astype(BF)

    def rows16(q):
        return pl.ds(pl.multiple_of(q * 16, 16), 16)

    def sum_copy(d):
        zz = lax.rem(z + d, NZ)
        return remote(
            es.at[lax.rem(zz, 2), rows16(lax.div(zz, 2))], er.at[z],
            esend.at[d - 1], erecv.at[d - 1], dev(dz=d),
        )

    for d in range(1, NZ):
        sum_copy(d).start()
    drains += [sum_copy(d) for d in range(1, NZ)]
    er[z] = es[zk, rows16(zq)]
    swaps[0].wait()
    hid = hidv[zk, pl.ds(pl.multiple_of(zq * 32, 32), 32), :].astype(F32)
    hid = jnp.concatenate(
        [jnp.where(core == 0, hid[8 * i:8 * i + 4], hid[8 * i + 4:8 * i + 8]) for i in range(4)],
        axis=0,
    )
    hid = jnp.concatenate([hid, jnp.zeros((16, 32), F32)], axis=1)
    for d in range(1, NZ):
        sum_copy(d).wait_recv()
    for b in range(NZ):
        hid = hid + er[b].astype(F32)
    state = hid.astype(BF).astype(F32)
    square = jnp.sum(state * state, axis=1, keepdims=True)
    high = square.astype(BF).astype(F32)
    lanes = lax.broadcasted_iota(jnp.int32, (16, 256), 1)
    state = jnp.where(lanes == 224, high, jnp.where(lanes == 225, square - high, state))
    unit = 2 * zk + lax.div(zq, 2)
    place = pl.ds(pl.multiple_of(16 * lax.rem(zq, 2), 16), 16)
    fg[x, y, unit, place] = state.astype(BF)

    def state_copy(d):
        ref = fg.at[x, y, unit, place]
        return remote(ref, ref, fsend.at[2, d - 1, 0], frecv.at[2, d - 1, 0], dev(dz=d))

    for d in range(1, NZ):
        state_copy(d).start()
    drains += [state_copy(d) for d in range(1, NZ)]
    for d in range(1, NZ):
        state_copy(d).wait_recv()
    drains += gatherer(fg, fsend, frecv)

    for c in big_loads[1:]:
        c.wait()
    for c in swaps[2:]:
        c.wait()

    def block(k, carry):
        h0, h1, tail = carry
        xx, yy, cc = lax.div(k, 8), lax.rem(lax.div(k, 2), 4), lax.rem(k, 2)
        v = fg[xx, yy, pl.ds(2 * cc, 2)].reshape(64, 256).astype(F32)
        tail = tail + v[:, 128:256]
        lhs = (v * gainv[pl.ds(k, 1), :]).astype(BF)
        return (h0 + dot(lhs, wguv[0, k]), h1 + dot(lhs, wguv[1, k]), tail)

    zero = jnp.zeros((64, 256), F32)
    h0, h1, tail = lax.fori_loop(0, 32, block, (zero, zero, jnp.zeros((64, 128), F32)))
    norm = lax.rsqrt((tail[:, 96:97] + tail[:, 97:98]) / 7168.0 + EPSILON)
    parts = []
    for k, h in enumerate((h0, h1)):
        gate, up = h[:, :128] * norm, h[:, 128:] * norm
        parts.append(gate / (1.0 + jnp.exp(-gate)) * up * gsel[:, 128 * k:128 * k + 128])
    active = jnp.concatenate(parts, axis=1)
    actf[...] = active
    for i in range(4):
        for j in range(4):
            actp[16 * j + 4 * i:16 * j + 4 * i + 4, :] = actf[16 * i + 4 * j:16 * i + 4 * j + 4, :]
    lhs = (active.astype(BF), actp[...].astype(BF))

    def scatterer(h, along_x, p_ref, m_ref, r_ref, send, recv):
        me = x if along_x else y

        def at(shift):
            return lax.rem(me + shift, 4)

        def copy(c):
            plus = c in (0, 2, 4)
            src, dst = [
                (p_ref.at[h, at(2), :, TOP], m_ref.at[h, 0]),
                (p_ref.at[h, at(2), :, BOT], m_ref.at[h, 1]),
                (p_ref.at[h, at(1), :, BOT], r_ref.at[h, 0, :, BOT]),
                (p_ref.at[h, at(3), :, TOP], r_ref.at[h, 1, :, TOP]),
                (p_ref.at[h, at(1), :, TOP], r_ref.at[h, 0, :, TOP]),
                (p_ref.at[h, at(3), :, BOT], r_ref.at[h, 1, :, BOT]),
            ][c]
            step = 1 if plus else 3
            target = dev(dx=step) if along_x else dev(dy=step)
            return remote(src, dst, send.at[h, c], recv.at[h, c], target)

        def begin():
            for c in range(4):
                copy(c).start()

        def middle():
            for c, shift, part in ((0, 1, TOP), (1, 3, BOT)):
                copy(c).wait_recv()
                joined = p_ref[h, at(shift), :, part].astype(F32) + m_ref[h, c].astype(F32)
                p_ref[h, at(shift), :, part] = joined.astype(p_ref.dtype)
                copy(4 + c).start()

        def end():
            for c in range(2, 6):
                copy(c).wait_recv()
            return (
                p_ref[h, me].astype(F32) + r_ref[h, 0].astype(F32) + r_ref[h, 1].astype(F32)
            )

        return begin, middle, end, [copy(c) for c in range(6)]

    first = [scatterer(h, h == 0, p1, m1, r1, hsend, hrecv) for h in range(2)]
    second = [scatterer(h, h == 1, p2, m2, r2, ssend, srecv) for h in range(2)]
    for h in range(2):
        for c in range(7):
            cols = pl.ds(h * HALF + 512 * c, 512)
            part = dot(lhs[h], wdv[:, cols]).astype(BF)
            p1[h, :, :, pl.ds(512 * c, 512)] = part.reshape(4, 16, 512)
        first[h][0]()
    for h in range(2):
        first[h][1]()
    for h in range(2):
        joined = first[h][2]()
        for i in range(4):
            p2[h, i] = joined[4 * i:4 * i + 4].astype(p2.dtype)
        second[h][0]()
    for h in range(2):
        second[h][1]()
    for h in range(2):
        joined = second[h][2]()
        for i in range(4):
            z3s[4 * h + i] = joined[:, 896 * i:896 * i + 896].astype(z3s.dtype)
        drains += first[h][3] + second[h][3]

    def last_copy(d):
        zz = lax.rem(z + d, NZ)
        return remote(z3s.at[zz], z3r.at[z], zsend.at[d - 1], zrecv.at[d - 1], dev(dz=d))

    for d in range(1, NZ):
        last_copy(d).start()
    drains += [last_copy(d) for d in range(1, NZ)]
    z3r[z] = z3s[z]

    pieces = []
    for i in range(4):
        pe = 2 * z + i // 2
        rows = fg[
            lax.div(pe, 4), lax.rem(pe, 4), 2 * (i % 2) + lax.div(x, 2),
            pl.ds(pl.multiple_of(16 * lax.rem(x, 2), 16), 16),
        ].astype(F32)
        picked = jnp.zeros((4, 256), F32)
        for j in range(4):
            picked = picked + jnp.where(y == j, rows[4 * j:4 * j + 4], 0.0)
        pieces.append(picked[:, :224])
    result = jnp.concatenate(pieces, axis=1)
    for d in range(1, NZ):
        last_copy(d).wait_recv()
    for b in range(NZ):
        result = result + z3r[b].astype(F32)
    out_ref[...] = result.astype(BF)
    for c in drains:
        c.wait_send()


def per_device(
    q_latent, q_rope, cache_latent, cache_rope, lengths, w_attn_out, hidden_in, norm_gain,
    w_gate, w_up, w_down, expert_ids, gate_weights,
):
    gain = jnp.pad(norm_gain.reshape(32, 224).astype(F32), ((0, 0), (0, 32)))
    anywhere = pl.BlockSpec(memory_space=pl.ANY)
    specs = [anywhere] * 13
    specs[4] = pl.BlockSpec(memory_space=pltpu.SMEM)
    vmem = pltpu.VMEM
    dma = pltpu.SemaphoreType.DMA
    scratch = [
        vmem((4, 128, 512), BF), vmem((4, 64, 128), BF), vmem((4, 512, 512), BF),
        vmem((4, 64, 512), BF), vmem((2, 16, 512, 224), BF), vmem((2, 128, 224), BF),
        vmem((32, 256), F32), vmem((2, 32, 256, 256), BF), vmem((256, 7168), BF),
        vmem((128, 8), jnp.int32), vmem((128, 8), F32),
        vmem((4, 128, 512), BF), vmem((8, 128), F32), vmem((8, 8, 128), F32),
        vmem((8, 4, 16, 512), BF), vmem((128, 128), F32), vmem((4, 4, 4, 16, 512), BF),
        vmem((4, 1024, 128), F32), vmem((8, 128), F32), vmem((2, 64, 256), BF),
        vmem((8, 16, 256), BF), vmem((4, 4, 4, 32, 256), BF), vmem((128, 256), F32),
        vmem((64, 256), F32), vmem((64, 256), F32), vmem((64, 256), F32),
        vmem((2, 4, 16, HALF), BF), vmem((2, 2, 16, PART), BF), vmem((2, 2, 16, HALF), BF),
        vmem((2, 4, 4, HALF), F32), vmem((2, 2, 4, PART), F32), vmem((2, 2, 4, HALF), F32),
        vmem((8, 4, 896), F32), vmem((8, 4, 896), F32),
        dma((24,)), dma((5,)), dma((5,)), dma((5, 7)), dma((5, 7)),
        dma((2, 5, 4)), dma((2, 5, 4)), dma((7,)), dma((7,)), dma((3, 7, 4)), dma((3, 7, 4)),
        dma((2, 6)), dma((2, 6)), dma((2, 6)), dma((2, 6)), dma((1,)), dma((1,)),
        dma((7,)), dma((7,)),
    ]
    return pl.pallas_call(
        kernel,
        out_shape=jax.ShapeDtypeStruct((4, 896), BF),
        in_specs=specs,
        out_specs=pl.BlockSpec(memory_space=pltpu.VMEM),
        scratch_shapes=scratch,
        compiler_params=pltpu.CompilerParams(
            collective_id=0, has_side_effects=True, vmem_limit_bytes=56 * 1024 * 1024
        ),
    )(
        q_latent, q_rope, cache_latent, cache_rope, lengths, w_attn_out, hidden_in, gain,
        w_gate.reshape(32, 224, 128), w_up.reshape(32, 224, 128), w_down.reshape(128, 7168),
        expert_ids, gate_weights,
    )


def solution(mesh):
    in_specs = (
        P("exp", None, None),
        P("exp", None, None),
        P("exp", "ctx", None),
        P("exp", None, "ctx"),
        P("exp"),
        P("ctx", None, "exp"),
        P(None, "exp"),
        P(),
        P("exp", None, "ctx"),
        P("exp", None, "ctx"),
        P("exp", "ctx", None),
        P(),
        P(),
    )
    return jax.shard_map(
        per_device, mesh=mesh, in_specs=in_specs, out_specs=P("exp", "ctx"), check_vma=False
    )
```

```python
import functools

import jax
import jax.numpy as jnp
from jax import lax
from jax.experimental import pallas as pl
from jax.experimental.pallas import tpu as pltpu
from jax.sharding import PartitionSpec as P

SCALE = 192.0 ** (-0.5)
MASKED = -1e30
EPSILON = 1e-06
MESH = pl.DeviceIdType.MESH
BF = jnp.bfloat16
F32 = jnp.float32
NZ, NX, NY = 8, 4, 4
HALF = 3584
PART = 1792
TOP = pl.ds(0, PART)
BOT = pl.ds(PART, PART)
ACROSS = (((1,), (1,)), ((), ()))


def dot(a, b, dims=(((1,), (0,)), ((), ()))):
    return lax.dot_general(a, b, dims, preferred_element_type=F32)


def kernel(
    q_hbm, qr_hbm, kc_hbm, kr_hbm, len_ref, wo_hbm, hid_hbm, gain_hbm, wg_hbm, wu_hbm, wd_hbm,
    ids_hbm, gw_hbm, out_ref,
    qv, qrv, kcv, krv, wov, hidv, gainv, wguv, wdv, idsv, gwv,
    vb, st_s, st_r, br, bm, bh, mg, alv, gbuf, gf, ef, es, er, fg, gds, gsel, actf, actp,
    p1, m1, r1, p2, m2, r2, z3s, z3r, gainf, gainp, hidt,
    lsem, psend, precv, bsend, brecv, gsend, grecv, esend, erecv, fsend, frecv, tsend, trecv,
    hsend, hrecv, ssend, srecv, zsend, zrecv,
):
    z = lax.axis_index("ctx")
    e = lax.axis_index("exp")
    core = lax.rem(e, 2)
    p = lax.div(e, 2)
    y = lax.rem(p, NY)
    x = lax.div(p, NY)
    zq, zk = lax.div(z, 2), lax.rem(z, 2)

    def dev(dz=0, dx=0, dy=0, other=False):
        c = (1 - core) if other else core
        xx, yy = lax.rem(x + dx, NX), lax.rem(y + dy, NY)
        return {"ctx": lax.rem(z + dz, NZ), "exp": (xx * NY + yy) * 2 + c}

    barrier = pltpu.get_barrier_semaphore()
    peers = [dev(dz=d) for d in range(1, NZ)]
    peers += [dev(dx=1), dev(dx=3), dev(dy=1), dev(dy=3), dev(other=True)]
    for peer in peers:
        pl.semaphore_signal(barrier, inc=1, device_id=peer, device_id_type=MESH)

    def load(src, dst, k):
        return pltpu.make_async_copy(src, dst, lsem.at[k])

    row_loads = []
    for r in range(4):
        row_loads.append([
            load(q_hbm.at[r], qv.at[r], 4 * r),
            load(kc_hbm.at[r], kcv.at[r], 4 * r + 1),
            load(qr_hbm.at[r], qrv.at[r], 4 * r + 2),
            load(kr_hbm.at[r], krv.at[r], 4 * r + 3),
        ])
        for c in row_loads[r]:
            c.start()
    own = pl.ds(pl.multiple_of(core * 128, 128), 128)
    small_loads = [
        load(ids_hbm, idsv, 16),
        load(gw_hbm, gwv, 17),
        load(gain_hbm, gainv, 18),
        load(hid_hbm, hidv.at[core], 19),
    ]
    big_loads = [
        load(wo_hbm, wov.at[core], 20),
        load(wg_hbm, wguv.at[core, :, pl.ds(0, 224), pl.ds(0, 128)], 21),
        load(wu_hbm, wguv.at[core, :, pl.ds(0, 224), pl.ds(128, 128)], 22),
        load(wd_hbm, wdv.at[own], 23),
    ]
    for c in small_loads + big_loads:
        c.start()
    wguv[:, :, 224:256, :] = jnp.zeros((2, 32, 32, 256), BF)

    pl.semaphore_wait(barrier, len(peers))

    def swap(src, dst, k):
        return pltpu.make_async_remote_copy(
            src_ref=src, dst_ref=dst, send_sem=psend.at[k], recv_sem=precv.at[k],
            device_id=dev(other=True), device_id_type=MESH,
        )

    swaps = [
        swap(hid_hbm, hidv.at[core], 0),
        swap(wo_hbm, wov.at[core], 1),
        swap(wg_hbm, wguv.at[core, :, pl.ds(0, 224), pl.ds(0, 128)], 2),
        swap(wu_hbm, wguv.at[core, :, pl.ds(0, 224), pl.ds(128, 128)], 3),
        swap(wd_hbm, wdv.at[own], 4),
    ]
    for c in swaps:
        c.start()

    def remote(src, dst, ss, rs, device):
        return pltpu.make_async_remote_copy(
            src_ref=src, dst_ref=dst, send_sem=ss, recv_sem=rs,
            device_id=device, device_id_type=MESH,
        )

    def heads_of(zz):
        return pl.ds(pl.multiple_of(zz * 16, 16), 16)

    left256, right256 = pl.ds(0, 256), pl.ds(256, 256)

    def value_copy(r, c):
        src, dst, d = [
            (vb.at[r, heads_of(lax.rem(z + 1, NZ))], br.at[0, r], 1),
            (vb.at[r, heads_of(lax.rem(z + 7, NZ))], br.at[1, r], 7),
            (vb.at[r, heads_of(lax.rem(z + 3, NZ))], bm.at[0, r], 1),
            (vb.at[r, heads_of(lax.rem(z + 5, NZ))], bm.at[1, r], 7),
            (vb.at[r, heads_of(lax.rem(z + 4, NZ)), left256], bh.at[0, r], 2),
            (vb.at[r, heads_of(lax.rem(z + 4, NZ)), right256], bh.at[1, r], 6),
            (mg.at[0, r], br.at[2, r], 2),
            (mg.at[1, r], br.at[3, r], 6),
        ][c]
        return remote(src, dst, bsend.at[r, c], brecv.at[r, c], dev(dz=d))

    def stat_copy(d):
        return remote(st_s, st_r.at[d], bsend.at[4, d], brecv.at[4, d], dev(dz=d))

    lane = lax.broadcasted_iota(jnp.int32, (128, 128), 1)
    position = z * 512 + lax.broadcasted_iota(jnp.int32, (128, 512), 1)
    stats = jnp.zeros((128, 128), F32)
    for r in range(4):
        for c in row_loads[r]:
            c.wait()
        keys = kcv[r]
        scores = dot(qv[r], keys, ACROSS)
        scores = (scores + dot(qrv[r], krv[r], (((0,), (0,)), ((), ())))) * SCALE
        visible = position < len_ref[r]
        scores = jnp.where(visible, scores, MASKED)
        top = jnp.max(scores, axis=1, keepdims=True)
        weights = jnp.where(visible, jnp.exp(scores - top), 0.0)
        total = jnp.sum(weights, axis=1, keepdims=True)
        value = dot(weights.astype(BF), keys)
        held = jnp.maximum(total, 1e-30)
        vb[r] = (value / held).astype(BF)
        lse = jnp.where(total > 0.0, top + jnp.log(held), MASKED)
        stats = jnp.where(lane == r, lse, stats)
        if r == 3:
            st_s[...] = jnp.transpose(stats)[0:8]
            for d in range(1, NZ):
                stat_copy(d).start()
        for c in (2, 3, 4, 5, 0, 1):
            value_copy(r, c).start()
    st_r[0] = st_s[...]

    for c in small_loads:
        c.wait()
    for k in range(2):
        named = jnp.where(idsv[...] == 2 * p + k, gwv[...], 0.0)
        named = jnp.broadcast_to(jnp.sum(named, axis=0, keepdims=True), (128, 128))
        gds[:, 128 * k:128 * k + 128] = jnp.transpose(named)
    gain = gainv[...].astype(F32)
    gainf[...] = gain
    gain = jnp.concatenate([gainf[pl.ds(t, 8, stride=7), :] for t in range(7)], axis=1)
    for k in range(4):
        gainp[8 * k:8 * k + 8, :] = jnp.concatenate(
            [gain[:, 224 * k:224 * k + 224], jnp.zeros((8, 32), F32)], axis=1
        )
    for i in range(16):
        gsel[4 * i:4 * i + 4, :] = jnp.where(
            core == 0, gds[8 * i:8 * i + 4, :], gds[8 * i + 4:8 * i + 8, :]
        )

    for d in range(1, NZ):
        stat_copy(d).wait_recv()
    s = st_r[...]
    a = jnp.exp(s - jnp.max(s, axis=0, keepdims=True))
    a = a / jnp.sum(a, axis=0, keepdims=True)
    a = jnp.concatenate([a.reshape(64, 128), jnp.zeros((64, 128), F32)], axis=0)
    alv[...] = jnp.transpose(a)
    share = [alv[heads_of(lax.rem(z + d, NZ)), :] for d in (0, 2, 6)]

    def scaled(which, d, r, block):
        return share[which][:, 8 * d + r:8 * d + r + 1] * block.astype(F32)

    for r in range(4):
        for c in (2, 3, 4, 5):
            value_copy(r, c).wait_recv()
        for k, near, far in ((0, 1, 2), (1, 7, 6)):
            to = heads_of(lax.rem(z + (6 if k else 2), NZ))
            joined = scaled(1 + k, 0, r, vb[r, to]) + scaled(1 + k, near, r, bm[k, r])
            half = scaled(1 + k, far, r, bh[k, r])
            pad = jnp.zeros((16, 256), F32)
            joined = joined + jnp.concatenate([half, pad] if k == 0 else [pad, half], axis=1)
            mg[k, r] = joined.astype(BF)
            value_copy(r, 6 + k).start()

    def combine(r):
        for c in (0, 1, 6, 7):
            value_copy(r, c).wait_recv()
        acc = scaled(0, 0, r, vb[r, heads_of(z)])
        acc = acc + scaled(0, 1, r, br[0, r]) + scaled(0, 7, r, br[1, r])
        acc = acc + br[2, r].astype(F32) + br[3, r].astype(F32)
        gbuf[x, y, r] = acc.astype(BF)

    def gatherer(buf, send, recv, x_first, both, forward):
        def region(g, i1, i2, part):
            i1, i2 = lax.rem(i1, 4), lax.rem(i2, 4)
            xx, yy = (i1, i2) if x_first(g) else (i2, i1)
            return buf.at[(xx, yy) + part]

        def copy(g, j, c):
            me1, me2 = (x, y) if x_first(g) else (y, x)
            step = 1 if c in (0, 2) else 3
            part = both(g) if c < 2 else forward(g, c - 2)
            shift = {0: 0, 1: 0, 2: 3, 3: 1}[c]
            if j == 4:
                ref = region(g, me1 + shift, me2, part)
                along_x = x_first(g)
            else:
                column = {0: 0, 1: 3, 2: 1, 3: 2}[j]
                ref = region(g, me1 + column, me2 + shift, part)
                along_x = not x_first(g)
            target = dev(dx=step) if along_x else dev(dy=step)
            return remote(ref, ref, send.at[g, j, c], recv.at[g, j, c], target)

        def place(g, j, i):
            me1, me2 = (x, y) if x_first(g) else (y, x)
            i1 = lax.rem(me1 + {0: 0, 1: 3, 2: 1, 3: 2}[j], 4)
            i2 = lax.rem(me2 + {0: 0, 1: 3, 2: 1, 3: 2}[i], 4)
            return (i1, i2) if x_first(g) else (i2, i1)

        def launch(g, j):
            copy(g, j, 0).start()
            copy(g, j, 1).start()

        def pass_on(g, j):
            for c in range(2):
                copy(g, j, c).wait_recv()
                copy(g, j, c + 2).start()
                if j == 4:
                    launch(g, 1 + c)

        def far(g, j):
            copy(g, j, 2).wait_recv()
            copy(g, j, 3).wait_recv()
            if j == 4:
                launch(g, 3)

        def stage(g, n):
            if n == 0:
                launch(g, 4)
                launch(g, 0)
                return [(0, 0)]
            if n == 1:
                pass_on(g, 4)
                return [(1, 0), (2, 0)]
            if n == 2:
                pass_on(g, 0)
                return [(0, 1), (0, 2)]
            if n == 3:
                far(g, 4)
                pass_on(g, 1)
                pass_on(g, 2)
                return [(3, 0), (1, 1), (1, 2), (2, 1), (2, 2)]
            if n == 4:
                pass_on(g, 3)
                far(g, 0)
                return [(0, 3), (3, 1), (3, 2)]
            far(g, 1)
            far(g, 2)
            far(g, 3)
            return [(1, 3), (2, 3), (3, 3)]

        def copies(groups):
            return [copy(g, j, c) for g in range(groups) for j in range(5) for c in range(4)]

        return stage, place, copies

    drains = [value_copy(r, c) for r in range(4) for c in range(8)]
    drains += [stat_copy(d) for d in range(1, NZ)]
    stage, _, copies = gatherer(
        gbuf, gsend, grecv, lambda g: g % 2 == 0, lambda g: (g,),
        lambda g, c: (g, slice(None), (left256, right256)[c]),
    )
    for t in range(9):
        for g in reversed(range(4)):
            if t == g:
                combine(g)
            if 0 <= t - g < 6:
                stage(g, t - g)
            if t - g == 5:
                for i in range(16):
                    rows = gbuf[i // 4, i % 4, g].astype(F32)
                    for k in range(4):
                        gf[k, 64 * i + 16 * g:64 * i + 16 * g + 16, :] = rows[:, 128 * k:128 * k + 128]
    drains += copies(4)

    big_loads[0].wait()
    swaps[1].wait()

    def head(h, accs):
        lhs = jnp.concatenate(
            [gf[t, pl.ds(h, 64, stride=16), :] for t in range(4)], axis=1
        ).astype(BF)
        return (accs[0] + dot(lhs, wov[0, h], ACROSS), accs[1] + dot(lhs, wov[1, h], ACROSS))

    accs = lax.fori_loop(0, 16, head, (jnp.zeros((64, 224), F32), jnp.zeros((64, 224), F32)))
    for k in range(2):
        es[k] = jnp.concatenate([accs[k], jnp.zeros((64, 32), F32)], axis=1).astype(BF)

    def rows16(q):
        return pl.ds(pl.multiple_of(q * 16, 16), 16)

    def sum_copy(d):
        zz = lax.rem(z + d, NZ)
        return remote(
            es.at[lax.rem(zz, 2), rows16(lax.div(zz, 2))], er.at[z],
            esend.at[d - 1], erecv.at[d - 1], dev(dz=d),
        )

    for d in range(1, NZ):
        sum_copy(d).start()
    drains += [sum_copy(d) for d in range(1, NZ)]
    er[z] = es[zk, rows16(zq)]
    swaps[0].wait()
    hid = jnp.concatenate([hidv[zk].astype(F32), jnp.zeros((32, 128), F32)], axis=0)
    hidt[...] = jnp.transpose(hid)
    hid = hidt[pl.ds(pl.multiple_of(zq * 32, 32), 32), :]
    hid = jnp.concatenate(
        [jnp.where(core == 0, hid[8 * i:8 * i + 4], hid[8 * i + 4:8 * i + 8]) for i in range(4)],
        axis=0,
    )
    for d in range(1, NZ):
        sum_copy(d).wait_recv()
    for b in range(NZ):
        hid = hid + er[b].astype(F32)
    state = hid.astype(BF).astype(F32)
    square = jnp.sum(state * state, axis=1, keepdims=True)
    high = square.astype(BF).astype(F32)
    lanes = lax.broadcasted_iota(jnp.int32, (16, 256), 1)
    state = jnp.where(lanes == 224, high, jnp.where(lanes == 225, square - high, state))
    unit = 2 * zk + lax.div(zq, 2)
    place = pl.ds(pl.multiple_of(16 * lax.rem(zq, 2), 16), 16)
    fg[x, y, unit, place] = state.astype(BF)

    def state_copy(d):
        ref = fg.at[x, y, unit, place]
        return remote(ref, ref, tsend.at[d - 1], trecv.at[d - 1], dev(dz=d))

    for d in range(1, NZ):
        state_copy(d).start()
    drains += [state_copy(d) for d in range(1, NZ)]
    for d in range(1, NZ):
        state_copy(d).wait_recv()
    for c in big_loads[1:]:
        c.wait()
    for c in swaps[2:]:
        c.wait()
    stage, place_of, copies = gatherer(
        fg, fsend, frecv, lambda g: g == 0, lambda g: (pl.ds(2 * g, 2),),
        lambda g, c: (2 * g + c,),
    )
    zero = jnp.zeros((64, 256), F32)
    h0, h1, tail = zero, zero, jnp.zeros((64, 128), F32)
    for n in range(6):
        blocks = [(g, b) for g in range(2) for b in stage(g, n)]
        for g, (j, i) in blocks:
            xx, yy = place_of(g, j, i)
            k = (xx * NY + yy) * 2 + g
            v = fg[xx, yy, pl.ds(2 * g, 2)].reshape(64, 256).astype(F32)
            tail = tail + v[:, 128:256]
            scale = gainp[pl.ds(8 * lax.rem(k, 4) + lax.div(k, 4), 1), :]
            lhs = (v * scale).astype(BF)
            h0 = h0 + dot(lhs, wguv[0, k])
            h1 = h1 + dot(lhs, wguv[1, k])
    drains += copies(2)

    norm = lax.rsqrt((tail[:, 96:97] + tail[:, 97:98]) / 7168.0 + EPSILON)
    parts = []
    for k, h in enumerate((h0, h1)):
        gate, up = h[:, :128] * norm, h[:, 128:] * norm
        parts.append(gate / (1.0 + jnp.exp(-gate)) * up * gsel[:, 128 * k:128 * k + 128])
    active = jnp.concatenate(parts, axis=1)
    actf[...] = active
    for i in range(4):
        for j in range(4):
            actp[16 * j + 4 * i:16 * j + 4 * i + 4, :] = actf[16 * i + 4 * j:16 * i + 4 * j + 4, :]
    lhs = (active.astype(BF), actp[...].astype(BF))

    def scatterer(h, along_x, p_ref, m_ref, r_ref, send, recv):
        me = x if along_x else y

        def at(shift):
            return lax.rem(me + shift, 4)

        def copy(c):
            plus = c in (0, 2, 4)
            src, dst = [
                (p_ref.at[h, at(2), :, TOP], m_ref.at[h, 0]),
                (p_ref.at[h, at(2), :, BOT], m_ref.at[h, 1]),
                (p_ref.at[h, at(1), :, BOT], r_ref.at[h, 0, :, BOT]),
                (p_ref.at[h, at(3), :, TOP], r_ref.at[h, 1, :, TOP]),
                (p_ref.at[h, at(1), :, TOP], r_ref.at[h, 0, :, TOP]),
                (p_ref.at[h, at(3), :, BOT], r_ref.at[h, 1, :, BOT]),
            ][c]
            step = 1 if plus else 3
            target = dev(dx=step) if along_x else dev(dy=step)
            return remote(src, dst, send.at[h, c], recv.at[h, c], target)

        def begin():
            for c in range(4):
                copy(c).start()

        def middle():
            for c, shift, part in ((0, 1, TOP), (1, 3, BOT)):
                copy(c).wait_recv()
                joined = p_ref[h, at(shift), :, part].astype(F32) + m_ref[h, c].astype(F32)
                p_ref[h, at(shift), :, part] = joined.astype(p_ref.dtype)
                copy(4 + c).start()

        def end():
            for c in range(2, 6):
                copy(c).wait_recv()
            return (
                p_ref[h, me].astype(F32) + r_ref[h, 0].astype(F32) + r_ref[h, 1].astype(F32)
            )

        return begin, middle, end, [copy(c) for c in range(6)]

    first = [scatterer(h, h == 0, p1, m1, r1, hsend, hrecv) for h in range(2)]
    second = [scatterer(h, h == 1, p2, m2, r2, ssend, srecv) for h in range(2)]
    for h in range(2):
        for c in range(7):
            cols = pl.ds(h * HALF + 512 * c, 512)
            part = dot(lhs[h], wdv[:, cols]).astype(BF)
            p1[h, :, :, pl.ds(512 * c, 512)] = part.reshape(4, 16, 512)
        first[h][0]()
    for h in range(2):
        first[h][1]()
    for h in range(2):
        joined = first[h][2]()
        for i in range(4):
            p2[h, i] = joined[4 * i:4 * i + 4].astype(p2.dtype)
        second[h][0]()
    for h in range(2):
        second[h][1]()
    for h in range(2):
        joined = second[h][2]()
        for i in range(4):
            z3s[4 * h + i] = joined[:, 896 * i:896 * i + 896].astype(z3s.dtype)
        drains += first[h][3] + second[h][3]

    def last_copy(d):
        zz = lax.rem(z + d, NZ)
        return remote(z3s.at[zz], z3r.at[z], zsend.at[d - 1], zrecv.at[d - 1], dev(dz=d))

    for d in range(1, NZ):
        last_copy(d).start()
    drains += [last_copy(d) for d in range(1, NZ)]
    z3r[z] = z3s[z]

    pieces = []
    for i in range(4):
        pe = 2 * z + i // 2
        rows = fg[
            lax.div(pe, 4), lax.rem(pe, 4), 2 * (i % 2) + lax.div(x, 2),
            pl.ds(pl.multiple_of(16 * lax.rem(x, 2), 16), 16),
        ].astype(F32)
        picked = jnp.zeros((4, 256), F32)
        for j in range(4):
            picked = picked + jnp.where(y == j, rows[4 * j:4 * j + 4], 0.0)
        pieces.append(picked[:, :224])
    result = jnp.concatenate(pieces, axis=1)
    for d in range(1, NZ):
        last_copy(d).wait_recv()
    for b in range(NZ):
        result = result + z3r[b].astype(F32)
    out_ref[...] = result.astype(BF)
    for c in drains:
        c.wait_send()


def per_device(
    q_latent, q_rope, cache_latent, cache_rope, lengths, w_attn_out, hidden_in, norm_gain,
    w_gate, w_up, w_down, expert_ids, gate_weights,
):
    anywhere = pl.BlockSpec(memory_space=pl.ANY)
    specs = [anywhere] * 13
    specs[4] = pl.BlockSpec(memory_space=pltpu.SMEM)
    vmem = pltpu.VMEM
    dma = pltpu.SemaphoreType.DMA
    scratch = [
        vmem((4, 128, 512), BF), vmem((4, 64, 128), BF), vmem((4, 512, 512), BF),
        vmem((4, 64, 512), BF), vmem((2, 16, 224, 512), BF), vmem((2, 224, 128), BF),
        vmem((56, 128), BF), vmem((2, 32, 256, 256), BF), vmem((256, 7168), BF),
        vmem((8, 128), jnp.int32), vmem((8, 128), F32),
        vmem((4, 128, 512), BF), vmem((8, 128), F32), vmem((8, 8, 128), F32),
        vmem((4, 4, 16, 512), BF), vmem((2, 4, 16, 512), BF), vmem((2, 4, 16, 256), BF),
        vmem((2, 4, 16, 512), BF), vmem((128, 128), F32), vmem((4, 4, 4, 16, 512), BF),
        vmem((4, 1024, 128), F32), vmem((8, 128), F32), vmem((2, 64, 256), BF),
        vmem((8, 16, 256), BF), vmem((4, 4, 4, 32, 256), BF), vmem((128, 256), F32),
        vmem((64, 256), F32), vmem((64, 256), F32), vmem((64, 256), F32),
        vmem((2, 4, 16, HALF), BF), vmem((2, 2, 16, PART), BF), vmem((2, 2, 16, HALF), BF),
        vmem((2, 4, 4, HALF), BF), vmem((2, 2, 4, PART), BF), vmem((2, 2, 4, HALF), BF),
        vmem((8, 4, 896), BF), vmem((8, 4, 896), BF), vmem((56, 128), F32),
        vmem((32, 256), F32), vmem((128, 256), F32),
        dma((24,)), dma((5,)), dma((5,)), dma((5, 8)), dma((5, 8)),
        dma((4, 5, 4)), dma((4, 5, 4)), dma((7,)), dma((7,)), dma((2, 5, 4)), dma((2, 5, 4)),
        dma((7,)), dma((7,)),
        dma((2, 6)), dma((2, 6)), dma((2, 6)), dma((2, 6)),
        dma((7,)), dma((7,)),
    ]
    return pl.pallas_call(
        kernel,
        out_shape=jax.ShapeDtypeStruct((4, 896), BF),
        in_specs=specs,
        out_specs=pl.BlockSpec(memory_space=pltpu.VMEM),
        scratch_shapes=scratch,
        compiler_params=pltpu.CompilerParams(
            collective_id=0, has_side_effects=True, vmem_limit_bytes=56 * 1024 * 1024
        ),
    )(
        q_latent, q_rope, cache_latent, cache_rope, lengths, jnp.swapaxes(w_attn_out, 1, 2),
        hidden_in.T, norm_gain.reshape(56, 128),
        w_gate.reshape(32, 224, 128), w_up.reshape(32, 224, 128), w_down.reshape(128, 7168),
        expert_ids.T, gate_weights.T,
    )


def solution(mesh):
    in_specs = (
        P("exp", None, None),
        P("exp", None, None),
        P("exp", "ctx", None),
        P("exp", None, "ctx"),
        P("exp"),
        P("ctx", None, "exp"),
        P(None, "exp"),
        P(),
        P("exp", None, "ctx"),
        P("exp", None, "ctx"),
        P("exp", "ctx", None),
        P(),
        P(),
    )
    return jax.shard_map(
        per_device, mesh=mesh, in_specs=in_specs, out_specs=P("exp", "ctx"), check_vma=False
    )
```

```python
import functools

import jax
import jax.numpy as jnp
from jax import lax
from jax.experimental import pallas as pl
from jax.experimental.pallas import tpu as pltpu
from jax.sharding import PartitionSpec as P

SCALE = 192.0 ** (-0.5)
MASKED = -1e30
EPSILON = 1e-06
MESH = pl.DeviceIdType.MESH
BF = jnp.bfloat16
F32 = jnp.float32
NZ, NX, NY = 8, 4, 4
HALF = 3584
WIDE = 1792
PART = 896
TOP = pl.ds(0, PART)
BOT = pl.ds(PART, PART)
ACROSS = (((1,), (1,)), ((), ()))


def dot(a, b, dims=(((1,), (0,)), ((), ()))):
    return lax.dot_general(a, b, dims, preferred_element_type=F32)


def kernel(
    q_hbm, qr_hbm, kc_hbm, kr_hbm, len_ref, wo_hbm, hid_hbm, gain_hbm, wg_hbm, wu_hbm, wd_hbm,
    ids_hbm, gw_hbm, out_ref,
    qv, qrv, kcv, krv, wov, hidv, gainv, wguv, wdv, idsv, gwv,
    vb, st_s, st_r, br, bm, bh, mg, alv, gbuf, gf, ef, es, er, fg, gds, gsel, actf, actp,
    p1, m1, r1, p2, m2, r2, z3s, z3r, gainf, gainp, hidt,
    lsem, psend, precv, bsend, brecv, gsend, grecv, esend, erecv, fsend, frecv, tsend, trecv,
    hsend, hrecv, ssend, srecv, zsend, zrecv,
):
    z = lax.axis_index("ctx")
    e = lax.axis_index("exp")
    core = lax.rem(e, 2)
    p = lax.div(e, 2)
    y = lax.rem(p, NY)
    x = lax.div(p, NY)
    zq, zk = lax.div(z, 2), lax.rem(z, 2)

    def dev(dz=0, dx=0, dy=0, other=False):
        c = (1 - core) if other else core
        xx, yy = lax.rem(x + dx, NX), lax.rem(y + dy, NY)
        return {"ctx": lax.rem(z + dz, NZ), "exp": (xx * NY + yy) * 2 + c}

    barrier = pltpu.get_barrier_semaphore()
    peers = [dev(dz=d) for d in range(1, NZ)]
    peers += [dev(dx=1), dev(dx=3), dev(dy=1), dev(dy=3), dev(other=True)]
    for peer in peers:
        pl.semaphore_signal(barrier, inc=1, device_id=peer, device_id_type=MESH)

    def load(src, dst, k):
        return pltpu.make_async_copy(src, dst, lsem.at[k])

    row_loads = []
    for r in range(4):
        row_loads.append([
            load(q_hbm.at[r], qv.at[r], 4 * r),
            load(kc_hbm.at[r], kcv.at[r], 4 * r + 1),
            load(qr_hbm.at[r], qrv.at[r], 4 * r + 2),
            load(kr_hbm.at[r], krv.at[r], 4 * r + 3),
        ])
        for c in row_loads[r]:
            c.start()
    own = pl.ds(pl.multiple_of(core * 128, 128), 128)
    small_loads = [
        load(ids_hbm, idsv, 16),
        load(gw_hbm, gwv, 17),
        load(gain_hbm, gainv, 18),
        load(hid_hbm, hidv.at[core], 19),
    ]
    big_loads = [
        load(wo_hbm, wov.at[core], 20),
        load(wg_hbm, wguv.at[core, :, pl.ds(0, 224), pl.ds(0, 128)], 21),
        load(wu_hbm, wguv.at[core, :, pl.ds(0, 224), pl.ds(128, 128)], 22),
        load(wd_hbm, wdv.at[own], 23),
    ]
    for c in small_loads + big_loads:
        c.start()
    wguv[:, :, 224:256, :] = jnp.zeros((2, 32, 32, 256), BF)

    pl.semaphore_wait(barrier, len(peers))

    def swap(src, dst, k):
        return pltpu.make_async_remote_copy(
            src_ref=src, dst_ref=dst, send_sem=psend.at[k], recv_sem=precv.at[k],
            device_id=dev(other=True), device_id_type=MESH,
        )

    swaps = [
        swap(hid_hbm, hidv.at[core], 0),
        swap(wo_hbm, wov.at[core], 1),
        swap(wg_hbm, wguv.at[core, :, pl.ds(0, 224), pl.ds(0, 128)], 2),
        swap(wu_hbm, wguv.at[core, :, pl.ds(0, 224), pl.ds(128, 128)], 3),
        swap(wd_hbm, wdv.at[own], 4),
    ]
    for c in swaps:
        c.start()

    def remote(src, dst, ss, rs, device):
        return pltpu.make_async_remote_copy(
            src_ref=src, dst_ref=dst, send_sem=ss, recv_sem=rs,
            device_id=device, device_id_type=MESH,
        )

    def heads_of(zz):
        return pl.ds(pl.multiple_of(zz * 16, 16), 16)

    left256, right256 = pl.ds(0, 256), pl.ds(256, 256)

    def value_copy(r, c):
        src, dst, d = [
            (vb.at[r, heads_of(lax.rem(z + 1, NZ))], br.at[0, r], 1),
            (vb.at[r, heads_of(lax.rem(z + 7, NZ))], br.at[1, r], 7),
            (vb.at[r, heads_of(lax.rem(z + 3, NZ))], bm.at[0, r], 1),
            (vb.at[r, heads_of(lax.rem(z + 5, NZ))], bm.at[1, r], 7),
            (vb.at[r, heads_of(lax.rem(z + 4, NZ)), left256], bh.at[0, r], 2),
            (vb.at[r, heads_of(lax.rem(z + 4, NZ)), right256], bh.at[1, r], 6),
            (mg.at[0, r], br.at[2, r], 2),
            (mg.at[1, r], br.at[3, r], 6),
        ][c]
        return remote(src, dst, bsend.at[r, c], brecv.at[r, c], dev(dz=d))

    def stat_copy(d):
        return remote(st_s, st_r.at[d], bsend.at[4, d], brecv.at[4, d], dev(dz=d))

    lane = lax.broadcasted_iota(jnp.int32, (128, 128), 1)
    position = z * 512 + lax.broadcasted_iota(jnp.int32, (128, 512), 1)
    stats = jnp.zeros((128, 128), F32)
    for r in range(4):
        for c in row_loads[r]:
            c.wait()
        keys = kcv[r]
        scores = dot(qv[r], keys, ACROSS)
        scores = (scores + dot(qrv[r], krv[r], (((0,), (0,)), ((), ())))) * SCALE
        visible = position < len_ref[r]
        scores = jnp.where(visible, scores, MASKED)
        top = jnp.max(scores, axis=1, keepdims=True)
        weights = jnp.where(visible, jnp.exp(scores - top), 0.0)
        total = jnp.sum(weights, axis=1, keepdims=True)
        value = dot(weights.astype(BF), keys)
        held = jnp.maximum(total, 1e-30)
        vb[r] = (value / held).astype(BF)
        lse = jnp.where(total > 0.0, top + jnp.log(held), MASKED)
        stats = jnp.where(lane == r, lse, stats)
        if r == 3:
            st_s[...] = jnp.transpose(stats)[0:8]
            for d in range(1, NZ):
                stat_copy(d).start()
        for c in (2, 3, 4, 5, 0, 1):
            value_copy(r, c).start()
    st_r[0] = st_s[...]

    for c in small_loads:
        c.wait()
    for k in range(2):
        named = jnp.where(idsv[...] == 2 * p + k, gwv[...], 0.0)
        named = jnp.broadcast_to(jnp.sum(named, axis=0, keepdims=True), (128, 128))
        gds[:, 128 * k:128 * k + 128] = jnp.transpose(named)
    gain = gainv[...].astype(F32)
    gainf[...] = gain
    gain = jnp.concatenate([gainf[pl.ds(t, 8, stride=7), :] for t in range(7)], axis=1)
    for k in range(4):
        gainp[8 * k:8 * k + 8, :] = jnp.concatenate(
            [gain[:, 224 * k:224 * k + 224], jnp.zeros((8, 32), F32)], axis=1
        )
    for i in range(16):
        gsel[4 * i:4 * i + 4, :] = jnp.where(
            core == 0, gds[8 * i:8 * i + 4, :], gds[8 * i + 4:8 * i + 8, :]
        )

    for d in range(1, NZ):
        stat_copy(d).wait_recv()
    s = st_r[...]
    a = jnp.exp(s - jnp.max(s, axis=0, keepdims=True))
    a = a / jnp.sum(a, axis=0, keepdims=True)
    a = jnp.concatenate([a.reshape(64, 128), jnp.zeros((64, 128), F32)], axis=0)
    alv[...] = jnp.transpose(a)
    share = [alv[heads_of(lax.rem(z + d, NZ)), :] for d in (0, 2, 6)]

    def scaled(which, d, r, block):
        return share[which][:, 8 * d + r:8 * d + r + 1] * block.astype(F32)

    for r in range(4):
        for c in (2, 3, 4, 5):
            value_copy(r, c).wait_recv()
        for k, near, far in ((0, 1, 2), (1, 7, 6)):
            to = heads_of(lax.rem(z + (6 if k else 2), NZ))
            joined = scaled(1 + k, 0, r, vb[r, to]) + scaled(1 + k, near, r, bm[k, r])
            half = scaled(1 + k, far, r, bh[k, r])
            pad = jnp.zeros((16, 256), F32)
            joined = joined + jnp.concatenate([half, pad] if k == 0 else [pad, half], axis=1)
            mg[k, r] = joined.astype(BF)
            value_copy(r, 6 + k).start()

    def combine(r):
        for c in (0, 1, 6, 7):
            value_copy(r, c).wait_recv()
        acc = scaled(0, 0, r, vb[r, heads_of(z)])
        acc = acc + scaled(0, 1, r, br[0, r]) + scaled(0, 7, r, br[1, r])
        acc = acc + br[2, r].astype(F32) + br[3, r].astype(F32)
        gbuf[x, y, r] = acc.astype(BF)

    def gatherer(buf, send, recv, x_first, both, forward):
        def region(g, i1, i2, part):
            i1, i2 = lax.rem(i1, 4), lax.rem(i2, 4)
            xx, yy = (i1, i2) if x_first(g) else (i2, i1)
            return buf.at[(xx, yy) + part]

        def copy(g, j, c):
            me1, me2 = (x, y) if x_first(g) else (y, x)
            step = 1 if c in (0, 2) else 3
            part = both(g) if c < 2 else forward(g, c - 2)
            shift = {0: 0, 1: 0, 2: 3, 3: 1}[c]
            if j == 4:
                ref = region(g, me1 + shift, me2, part)
                along_x = x_first(g)
            else:
                column = {0: 0, 1: 3, 2: 1, 3: 2}[j]
                ref = region(g, me1 + column, me2 + shift, part)
                along_x = not x_first(g)
            target = dev(dx=step) if along_x else dev(dy=step)
            return remote(ref, ref, send.at[g, j, c], recv.at[g, j, c], target)

        def place(g, j, i):
            me1, me2 = (x, y) if x_first(g) else (y, x)
            i1 = lax.rem(me1 + {0: 0, 1: 3, 2: 1, 3: 2}[j], 4)
            i2 = lax.rem(me2 + {0: 0, 1: 3, 2: 1, 3: 2}[i], 4)
            return (i1, i2) if x_first(g) else (i2, i1)

        def launch(g, j):
            copy(g, j, 0).start()
            copy(g, j, 1).start()

        def pass_on(g, j):
            for c in range(2):
                copy(g, j, c).wait_recv()
                copy(g, j, c + 2).start()
                if j == 4:
                    launch(g, 1 + c)

        def far(g, j):
            copy(g, j, 2).wait_recv()
            copy(g, j, 3).wait_recv()
            if j == 4:
                launch(g, 3)

        def stage(g, n):
            if n == 0:
                launch(g, 4)
                launch(g, 0)
            elif n == 1:
                pass_on(g, 4)
            elif n == 2:
                pass_on(g, 0)
            elif n == 3:
                far(g, 4)
                pass_on(g, 1)
                pass_on(g, 2)
            elif n == 4:
                pass_on(g, 3)
            elif n == 5:
                far(g, 0)
            elif n == 6:
                far(g, 1)
                far(g, 2)
            else:
                far(g, 3)

        def copies(groups):
            return [copy(g, j, c) for g in range(groups) for j in range(5) for c in range(4)]

        return stage, place, copies

    drains = [value_copy(r, c) for r in range(4) for c in range(8)]
    drains += [stat_copy(d) for d in range(1, NZ)]
    stage, place_of, copies = gatherer(
        gbuf, gsend, grecv, lambda g: g == 0, lambda g: (pl.ds(2 * g, 2),),
        lambda g, c: (2 * g + c,),
    )

    def spread(blocks):
        for g, (j, i) in blocks:
            xx, yy = place_of(g, j, i)
            for r in (2 * g, 2 * g + 1):
                rows = gbuf[xx, yy, r].astype(F32)
                at = pl.ds(pl.multiple_of((4 * (xx * NY + yy) + r) * 24, 8), 16)
                for k in range(4):
                    gf[k, at, :] = rows[:, 128 * k:128 * k + 128]

    def run_gather(stage, use):
        own = [(0, 0)]
        for g in range(2):
            stage(g, 0)
        use([(g, b) for g in range(2) for b in own])
        for n, ready in (
            (1, []), (2, [(1, 0), (2, 0), (0, 1)]), (3, [(0, 2), (3, 0), (1, 1), (1, 2)]),
            (4, [(2, 1), (2, 2), (3, 1), (3, 2)]), (5, [(0, 3)]), (6, [(1, 3), (2, 3)]),
            (7, [(3, 3)]),
        ):
            for g in range(2):
                stage(g, n)
            use([(g, b) for g in range(2) for b in ready])

    for r in range(4):
        combine(r)
    run_gather(stage, spread)
    drains += copies(2)

    big_loads[0].wait()
    swaps[1].wait()

    def head(h, accs):
        lhs = jnp.concatenate(
            [gf[t, pl.ds(h, 64, stride=24), :] for t in range(4)], axis=1
        ).astype(BF)
        return (accs[0] + dot(lhs, wov[0, h], ACROSS), accs[1] + dot(lhs, wov[1, h], ACROSS))

    accs = lax.fori_loop(0, 16, head, (jnp.zeros((64, 224), F32), jnp.zeros((64, 224), F32)), unroll=4)
    for k in range(2):
        es[k] = jnp.concatenate([accs[k], jnp.zeros((64, 32), F32)], axis=1).astype(BF)

    def rows16(q):
        return pl.ds(pl.multiple_of(q * 16, 16), 16)

    def sum_copy(d):
        zz = lax.rem(z + d, NZ)
        return remote(
            es.at[lax.rem(zz, 2), rows16(lax.div(zz, 2))], er.at[z],
            esend.at[d - 1], erecv.at[d - 1], dev(dz=d),
        )

    for d in range(1, NZ):
        sum_copy(d).start()
    drains += [sum_copy(d) for d in range(1, NZ)]
    er[z] = es[zk, rows16(zq)]
    swaps[0].wait()
    hid = jnp.concatenate([hidv[zk].astype(F32), jnp.zeros((32, 128), F32)], axis=0)
    hidt[...] = jnp.transpose(hid)
    hid = hidt[pl.ds(pl.multiple_of(zq * 32, 32), 32), :]
    hid = jnp.concatenate(
        [jnp.where(core == 0, hid[8 * i:8 * i + 4], hid[8 * i + 4:8 * i + 8]) for i in range(4)],
        axis=0,
    )
    for d in range(1, NZ):
        sum_copy(d).wait_recv()
    for b in range(NZ):
        hid = hid + er[b].astype(F32)
    state = hid.astype(BF).astype(F32)
    square = jnp.sum(state * state, axis=1, keepdims=True)
    high = square.astype(BF).astype(F32)
    lanes = lax.broadcasted_iota(jnp.int32, (16, 256), 1)
    state = jnp.where(lanes == 224, high, jnp.where(lanes == 225, square - high, state))
    unit = 2 * zk + lax.div(zq, 2)
    place = pl.ds(pl.multiple_of(16 * lax.rem(zq, 2), 16), 16)
    fg[x, y, unit, place] = state.astype(BF)

    def state_copy(d):
        ref = fg.at[x, y, unit, place]
        return remote(ref, ref, tsend.at[d - 1], trecv.at[d - 1], dev(dz=d))

    for d in range(1, NZ):
        state_copy(d).start()
    drains += [state_copy(d) for d in range(1, NZ)]
    for d in range(1, NZ):
        state_copy(d).wait_recv()
    for c in big_loads[1:]:
        c.wait()
    for c in swaps[2:]:
        c.wait()
    stage, place_of, copies = gatherer(
        fg, fsend, frecv, lambda g: g == 0, lambda g: (pl.ds(2 * g, 2),),
        lambda g, c: (2 * g + c,),
    )
    zero = jnp.zeros((64, 256), F32)
    sums = [zero, zero, jnp.zeros((64, 128), F32)]

    def multiply(blocks):
        for g, (j, i) in blocks:
            xx, yy = place_of(g, j, i)
            k = (xx * NY + yy) * 2 + g
            v = fg[xx, yy, pl.ds(2 * g, 2)].reshape(64, 256).astype(F32)
            scale = gainp[pl.ds(8 * lax.rem(k, 4) + lax.div(k, 4), 1), :]
            lhs = (v * scale).astype(BF)
            sums[0] = sums[0] + dot(lhs, wguv[0, k])
            sums[1] = sums[1] + dot(lhs, wguv[1, k])
            sums[2] = sums[2] + v[:, 128:256]

    run_gather(stage, multiply)
    h0, h1, tail = sums
    drains += copies(2)

    norm = lax.rsqrt((tail[:, 96:97] + tail[:, 97:98]) / 7168.0 + EPSILON)
    parts = []
    for k, h in enumerate((h0, h1)):
        gate, up = h[:, :128] * norm, h[:, 128:] * norm
        parts.append(gate / (1.0 + jnp.exp(-gate)) * up * gsel[:, 128 * k:128 * k + 128])
    active = jnp.concatenate(parts, axis=1)
    actf[...] = active
    for i in range(4):
        for j in range(4):
            actp[16 * j + 4 * i:16 * j + 4 * i + 4, :] = actf[16 * i + 4 * j:16 * i + 4 * j + 4, :]
    lhs = (active.astype(BF), actp[...].astype(BF))

    def scatterer(h, along_x, p_ref, m_ref, r_ref, send, recv):
        me = x if along_x else y

        def at(shift):
            return lax.rem(me + shift, 4)

        def copy(c):
            plus = c in (0, 2, 4)
            src, dst = [
                (p_ref.at[h, at(2), :, TOP], m_ref.at[h, 0]),
                (p_ref.at[h, at(2), :, BOT], m_ref.at[h, 1]),
                (p_ref.at[h, at(1), :, BOT], r_ref.at[h, 0, :, BOT]),
                (p_ref.at[h, at(3), :, TOP], r_ref.at[h, 1, :, TOP]),
                (p_ref.at[h, at(1), :, TOP], r_ref.at[h, 0, :, TOP]),
                (p_ref.at[h, at(3), :, BOT], r_ref.at[h, 1, :, BOT]),
            ][c]
            step = 1 if plus else 3
            target = dev(dx=step) if along_x else dev(dy=step)
            return remote(src, dst, send.at[h, c], recv.at[h, c], target)

        def begin():
            for c in range(4):
                copy(c).start()

        def middle():
            for c, shift, part in ((0, 1, TOP), (1, 3, BOT)):
                copy(c).wait_recv()
                joined = p_ref[h, at(shift), :, part].astype(F32) + m_ref[h, c].astype(F32)
                p_ref[h, at(shift), :, part] = joined.astype(p_ref.dtype)
                copy(4 + c).start()

        def end():
            for c in range(2, 6):
                copy(c).wait_recv()
            return (
                p_ref[h, me].astype(F32) + r_ref[h, 0].astype(F32) + r_ref[h, 1].astype(F32)
            )

        return begin, middle, end, [copy(c) for c in range(6)]

    groups = range(4)
    first = [scatterer(g, g % 2 == 0, p1, m1, r1, hsend, hrecv) for g in groups]
    second = [scatterer(g, g % 2 == 1, p2, m2, r2, ssend, srecv) for g in groups]
    for g in groups:
        base = (g % 2) * HALF + (g // 2) * WIDE
        for c in range(7):
            part = dot(lhs[g % 2], wdv[:, base + 256 * c:base + 256 * c + 256]).astype(BF)
            p1[g, :, :, 256 * c:256 * c + 256] = part.reshape(4, 16, 256)
        first[g][0]()
    for g in groups:
        first[g][1]()
    for g in groups:
        joined = first[g][2]()
        for i in range(4):
            p2[g, i] = joined[4 * i:4 * i + 4].astype(p2.dtype)
        second[g][0]()
    for g in groups:
        second[g][1]()
    for g in groups:
        joined = second[g][2]()
        for i in range(2):
            z3s[(g % 2) * 4 + (g // 2) * 2 + i] = joined[:, 896 * i:896 * i + 896].astype(z3s.dtype)
        drains += first[g][3] + second[g][3]

    def last_copy(d):
        zz = lax.rem(z + d, NZ)
        return remote(z3s.at[zz], z3r.at[z], zsend.at[d - 1], zrecv.at[d - 1], dev(dz=d))

    for d in range(1, NZ):
        last_copy(d).start()
    drains += [last_copy(d) for d in range(1, NZ)]
    z3r[z] = z3s[z]

    pieces = []
    for i in range(4):
        pe = 2 * z + i // 2
        rows = fg[
            lax.div(pe, 4), lax.rem(pe, 4), 2 * (i % 2) + lax.div(x, 2),
            pl.ds(pl.multiple_of(16 * lax.rem(x, 2), 16), 16),
        ].astype(F32)
        picked = jnp.zeros((4, 256), F32)
        for j in range(4):
            picked = picked + jnp.where(y == j, rows[4 * j:4 * j + 4], 0.0)
        pieces.append(picked[:, :224])
    result = jnp.concatenate(pieces, axis=1)
    for d in range(1, NZ):
        last_copy(d).wait_recv()
    for b in range(NZ):
        result = result + z3r[b].astype(F32)
    out_ref[...] = result.astype(BF)
    for c in drains:
        c.wait_send()


def per_device(
    q_latent, q_rope, cache_latent, cache_rope, lengths, w_attn_out, hidden_in, norm_gain,
    w_gate, w_up, w_down, expert_ids, gate_weights,
):
    anywhere = pl.BlockSpec(memory_space=pl.ANY)
    specs = [anywhere] * 13
    specs[4] = pl.BlockSpec(memory_space=pltpu.SMEM)
    vmem = pltpu.VMEM
    dma = pltpu.SemaphoreType.DMA
    scratch = [
        vmem((4, 128, 512), BF), vmem((4, 64, 128), BF), vmem((4, 512, 512), BF),
        vmem((4, 64, 512), BF), vmem((2, 16, 224, 512), BF), vmem((2, 224, 128), BF),
        vmem((56, 128), BF), vmem((2, 32, 256, 256), BF), vmem((256, 7168), BF),
        vmem((8, 128), jnp.int32), vmem((8, 128), F32),
        vmem((4, 128, 512), BF), vmem((8, 128), F32), vmem((8, 8, 128), F32),
        vmem((4, 4, 16, 512), BF), vmem((2, 4, 16, 512), BF), vmem((2, 4, 16, 256), BF),
        vmem((2, 4, 16, 512), BF), vmem((128, 128), F32), vmem((4, 4, 4, 16, 512), BF),
        vmem((4, 1536, 128), F32), vmem((8, 128), F32), vmem((2, 64, 256), BF),
        vmem((8, 16, 256), BF), vmem((4, 4, 4, 32, 256), BF), vmem((128, 256), F32),
        vmem((64, 256), F32), vmem((64, 256), F32), vmem((64, 256), F32),
        vmem((4, 4, 16, WIDE), BF), vmem((4, 2, 16, PART), BF), vmem((4, 2, 16, WIDE), BF),
        vmem((4, 4, 4, WIDE), BF), vmem((4, 2, 4, PART), BF), vmem((4, 2, 4, WIDE), BF),
        vmem((8, 4, 896), BF), vmem((8, 4, 896), BF), vmem((56, 128), F32),
        vmem((32, 256), F32), vmem((128, 256), F32),
        dma((24,)), dma((5,)), dma((5,)), dma((5, 8)), dma((5, 8)),
        dma((2, 5, 4)), dma((2, 5, 4)), dma((7,)), dma((7,)), dma((2, 5, 4)), dma((2, 5, 4)),
        dma((7,)), dma((7,)),
        dma((4, 6)), dma((4, 6)), dma((4, 6)), dma((4, 6)),
        dma((7,)), dma((7,)),
    ]
    return pl.pallas_call(
        kernel,
        out_shape=jax.ShapeDtypeStruct((4, 896), BF),
        in_specs=specs,
        out_specs=pl.BlockSpec(memory_space=pltpu.VMEM),
        scratch_shapes=scratch,
        compiler_params=pltpu.CompilerParams(
            collective_id=0, has_side_effects=True, vmem_limit_bytes=56 * 1024 * 1024
        ),
    )(
        q_latent, q_rope, cache_latent, cache_rope, lengths, jnp.swapaxes(w_attn_out, 1, 2),
        hidden_in.T, norm_gain.reshape(56, 128),
        w_gate.reshape(32, 224, 128), w_up.reshape(32, 224, 128), w_down.reshape(128, 7168),
        expert_ids.T, gate_weights.T,
    )


def solution(mesh):
    in_specs = (
        P("exp", None, None),
        P("exp", None, None),
        P("exp", "ctx", None),
        P("exp", None, "ctx"),
        P("exp"),
        P("ctx", None, "exp"),
        P(None, "exp"),
        P(),
        P("exp", None, "ctx"),
        P("exp", None, "ctx"),
        P("exp", "ctx", None),
        P(),
        P(),
    )
    return jax.shard_map(
        per_device, mesh=mesh, in_specs=in_specs, out_specs=P("exp", "ctx"), check_vma=False
    )
```

```python
import functools

import jax
import jax.numpy as jnp
from jax import lax
from jax.experimental import pallas as pl
from jax.experimental.pallas import tpu as pltpu
from jax.sharding import PartitionSpec as P

SCALE = 192.0 ** (-0.5)
MASKED = -1e30
EPSILON = 1e-06
MESH = pl.DeviceIdType.MESH
BF = jnp.bfloat16
F32 = jnp.float32
NZ, NX, NY = 8, 4, 4
HALF = 3584
WIDE = 1792
PART = 896
TOP = pl.ds(0, PART)
BOT = pl.ds(PART, PART)
ACROSS = (((1,), (1,)), ((), ()))


def dot(a, b, dims=(((1,), (0,)), ((), ()))):
    return lax.dot_general(a, b, dims, preferred_element_type=F32)


def kernel(
    q_hbm, qr_hbm, kc_hbm, kr_hbm, len_ref, wo_hbm, hid_hbm, gain_hbm, wg_hbm, wu_hbm, wd_hbm,
    ids_hbm, gw_hbm, out_ref,
    qv, qrv, kcv, krv, wov, hidv, gainv, wguv, wdv, idsv, gwv,
    vb, st_s, st_r, br, bm, bh, mg, alv, gbuf, gf, ef, es, er, fg, gds, gsel, actf, actp,
    p1, m1, r1, p2, r2, z3s, z3r, gainf, gainp, hidt,
    lsem, psend, precv, bsend, brecv, gsend, grecv, esend, erecv, fsend, frecv, tsend, trecv,
    hsend, hrecv, ssend, srecv, zsend, zrecv,
):
    z = lax.axis_index("ctx")
    e = lax.axis_index("exp")
    core = lax.rem(e, 2)
    p = lax.div(e, 2)
    y = lax.rem(p, NY)
    x = lax.div(p, NY)
    zq, zk = lax.div(z, 2), lax.rem(z, 2)

    def dev(dz=0, dx=0, dy=0, other=False):
        c = (1 - core) if other else core
        xx, yy = lax.rem(x + dx, NX), lax.rem(y + dy, NY)
        return {"ctx": lax.rem(z + dz, NZ), "exp": (xx * NY + yy) * 2 + c}

    barrier = pltpu.get_barrier_semaphore()
    peers = [dev(dz=d) for d in range(1, NZ)]
    peers += [dev(dx=d) for d in range(1, NX)] + [dev(dy=d) for d in range(1, NY)]
    peers += [dev(other=True)]
    for peer in peers:
        pl.semaphore_signal(barrier, inc=1, device_id=peer, device_id_type=MESH)

    def load(src, dst, k):
        return pltpu.make_async_copy(src, dst, lsem.at[k])

    row_loads = []
    for r in range(4):
        row_loads.append([
            load(q_hbm.at[r], qv.at[r], 4 * r),
            load(kc_hbm.at[r], kcv.at[r], 4 * r + 1),
            load(qr_hbm.at[r], qrv.at[r], 4 * r + 2),
            load(kr_hbm.at[r], krv.at[r], 4 * r + 3),
        ])
        for c in row_loads[r]:
            c.start()
    own = pl.ds(pl.multiple_of(core * 128, 128), 128)
    small_loads = [
        load(ids_hbm, idsv, 16),
        load(gw_hbm, gwv, 17),
        load(gain_hbm, gainv, 18),
        load(hid_hbm, hidv.at[core], 19),
    ]
    big_loads = [
        load(wo_hbm, wov.at[core], 20),
        load(wg_hbm, wguv.at[core, :, pl.ds(0, 224), pl.ds(0, 128)], 21),
        load(wu_hbm, wguv.at[core, :, pl.ds(0, 224), pl.ds(128, 128)], 22),
        load(wd_hbm, wdv.at[own], 23),
    ]
    for c in small_loads + big_loads:
        c.start()
    wguv[:, :, 224:256, :] = jnp.zeros((2, 32, 32, 256), BF)

    pl.semaphore_wait(barrier, len(peers))

    def swap(src, dst, k):
        return pltpu.make_async_remote_copy(
            src_ref=src, dst_ref=dst, send_sem=psend.at[k], recv_sem=precv.at[k],
            device_id=dev(other=True), device_id_type=MESH,
        )

    swaps = [
        swap(hid_hbm, hidv.at[core], 0),
        swap(wo_hbm, wov.at[core], 1),
        swap(wg_hbm, wguv.at[core, :, pl.ds(0, 224), pl.ds(0, 128)], 2),
        swap(wu_hbm, wguv.at[core, :, pl.ds(0, 224), pl.ds(128, 128)], 3),
        swap(wd_hbm, wdv.at[own], 4),
    ]
    for c in swaps:
        c.start()

    def remote(src, dst, ss, rs, device):
        return pltpu.make_async_remote_copy(
            src_ref=src, dst_ref=dst, send_sem=ss, recv_sem=rs,
            device_id=device, device_id_type=MESH,
        )

    def heads_of(zz):
        return pl.ds(pl.multiple_of(zz * 16, 16), 16)

    left256, right256 = pl.ds(0, 256), pl.ds(256, 256)

    def value_copy(r, c):
        src, dst, d = [
            (vb.at[r, heads_of(lax.rem(z + 1, NZ))], br.at[0, r], 1),
            (vb.at[r, heads_of(lax.rem(z + 7, NZ))], br.at[1, r], 7),
            (vb.at[r, heads_of(lax.rem(z + 3, NZ))], bm.at[0, r], 1),
            (vb.at[r, heads_of(lax.rem(z + 5, NZ))], bm.at[1, r], 7),
            (vb.at[r, heads_of(lax.rem(z + 4, NZ)), left256], bh.at[0, r], 2),
            (vb.at[r, heads_of(lax.rem(z + 4, NZ)), right256], bh.at[1, r], 6),
            (mg.at[0, r], br.at[2, r], 2),
            (mg.at[1, r], br.at[3, r], 6),
        ][c]
        return remote(src, dst, bsend.at[r, c], brecv.at[r, c], dev(dz=d))

    def stat_copy(d):
        return remote(st_s, st_r.at[d], bsend.at[4, d], brecv.at[4, d], dev(dz=d))

    lane = lax.broadcasted_iota(jnp.int32, (128, 128), 1)
    position = z * 512 + lax.broadcasted_iota(jnp.int32, (128, 512), 1)
    stats = jnp.zeros((128, 128), F32)
    for r in range(4):
        for c in row_loads[r]:
            c.wait()
        keys = kcv[r]
        scores = dot(qv[r], keys, ACROSS)
        scores = (scores + dot(qrv[r], krv[r], (((0,), (0,)), ((), ())))) * SCALE
        visible = position < len_ref[r]
        scores = jnp.where(visible, scores, MASKED)
        top = jnp.max(scores, axis=1, keepdims=True)
        weights = jnp.where(visible, jnp.exp(scores - top), 0.0)
        total = jnp.sum(weights, axis=1, keepdims=True)
        value = dot(weights.astype(BF), keys)
        held = jnp.maximum(total, 1e-30)
        vb[r] = (value / held).astype(BF)
        lse = jnp.where(total > 0.0, top + jnp.log(held), MASKED)
        stats = jnp.where(lane == r, lse, stats)
        if r == 3:
            st_s[...] = jnp.transpose(stats)[0:8]
            for d in range(1, NZ):
                stat_copy(d).start()
        for c in (2, 3, 4, 5, 0, 1):
            value_copy(r, c).start()
    st_r[0] = st_s[...]

    for c in small_loads:
        c.wait()
    for k in range(2):
        named = jnp.where(idsv[...] == 2 * p + k, gwv[...], 0.0)
        named = jnp.broadcast_to(jnp.sum(named, axis=0, keepdims=True), (128, 128))
        gds[:, 128 * k:128 * k + 128] = jnp.transpose(named)
    gain = gainv[...].astype(F32)
    gainf[0:56, :] = gain
    gain = jnp.concatenate([gainf[pl.ds(t, 8, stride=7), :] for t in range(7)], axis=1)
    for k in range(4):
        gainp[8 * k:8 * k + 8, :] = jnp.concatenate(
            [gain[:, 224 * k:224 * k + 224], jnp.zeros((8, 32), F32)], axis=1
        )
    for i in range(16):
        gsel[4 * i:4 * i + 4, :] = jnp.where(
            core == 0, gds[8 * i:8 * i + 4, :], gds[8 * i + 4:8 * i + 8, :]
        )

    for d in range(1, NZ):
        stat_copy(d).wait_recv()
    s = st_r[...]
    a = jnp.exp(s - jnp.max(s, axis=0, keepdims=True))
    a = a / jnp.sum(a, axis=0, keepdims=True)
    a = jnp.concatenate([a.reshape(64, 128), jnp.zeros((64, 128), F32)], axis=0)
    alv[...] = jnp.transpose(a)
    share = [alv[heads_of(lax.rem(z + d, NZ)), :] for d in (0, 2, 6)]

    def scaled(which, d, r, block):
        return share[which][:, 8 * d + r:8 * d + r + 1] * block.astype(F32)

    for r in range(4):
        for c in (2, 3, 4, 5):
            value_copy(r, c).wait_recv()
        for k, near, far in ((0, 1, 2), (1, 7, 6)):
            to = heads_of(lax.rem(z + (6 if k else 2), NZ))
            joined = scaled(1 + k, 0, r, vb[r, to]) + scaled(1 + k, near, r, bm[k, r])
            half = scaled(1 + k, far, r, bh[k, r])
            pad = jnp.zeros((16, 256), F32)
            joined = joined + jnp.concatenate([half, pad] if k == 0 else [pad, half], axis=1)
            mg[k, r] = joined.astype(BF)
            value_copy(r, 6 + k).start()

    def combine(r):
        for c in (0, 1, 6, 7):
            value_copy(r, c).wait_recv()
        acc = scaled(0, 0, r, vb[r, heads_of(z)])
        acc = acc + scaled(0, 1, r, br[0, r]) + scaled(0, 7, r, br[1, r])
        acc = acc + br[2, r].astype(F32) + br[3, r].astype(F32)
        gbuf[x, y, r] = acc.astype(BF)

    def gatherer(buf, send, recv, x_first, both, forward):
        def region(g, i1, i2, part):
            i1, i2 = lax.rem(i1, 4), lax.rem(i2, 4)
            xx, yy = (i1, i2) if x_first(g) else (i2, i1)
            return buf.at[(xx, yy) + part]

        def copy(g, j, c):
            me1, me2 = (x, y) if x_first(g) else (y, x)
            step = 1 if c in (0, 2) else 3
            part = both(g) if c < 2 else forward(g, c - 2)
            shift = {0: 0, 1: 0, 2: 3, 3: 1}[c]
            if j == 4 and c == 2:
                step, part, shift = 2, both(g), 0
            if j == 4:
                ref = region(g, me1 + shift, me2, part)
                along_x = x_first(g)
            else:
                column = {0: 0, 1: 3, 2: 1, 3: 2}[j]
                ref = region(g, me1 + column, me2 + shift, part)
                along_x = not x_first(g)
            target = dev(dx=step) if along_x else dev(dy=step)
            return remote(ref, ref, send.at[g, j, c], recv.at[g, j, c], target)

        def place(g, j, i):
            me1, me2 = (x, y) if x_first(g) else (y, x)
            i1 = lax.rem(me1 + {0: 0, 1: 3, 2: 1, 3: 2}[j], 4)
            i2 = lax.rem(me2 + {0: 0, 1: 3, 2: 1, 3: 2}[i], 4)
            return (i1, i2) if x_first(g) else (i2, i1)

        def launch(g, j):
            for c in range(3 if j == 4 else 2):
                copy(g, j, c).start()

        def pass_on(g, j):
            for c in range(2):
                copy(g, j, c).wait_recv()
                if j == 4:
                    launch(g, 1 + c)
                else:
                    copy(g, j, c + 2).start()

        def far(g, j):
            copy(g, j, 2).wait_recv()
            if j == 4:
                launch(g, 3)
            else:
                copy(g, j, 3).wait_recv()

        def stage(g, n):
            if n == 0:
                launch(g, 4)
                launch(g, 0)
            elif n == 1:
                pass_on(g, 4)
            elif n == 2:
                pass_on(g, 0)
            elif n == 3:
                far(g, 4)
                pass_on(g, 1)
                pass_on(g, 2)
            elif n == 4:
                pass_on(g, 3)
            elif n == 5:
                far(g, 0)
            elif n == 6:
                far(g, 1)
                far(g, 2)
            else:
                far(g, 3)

        def copies(groups):
            return [
                copy(g, j, c)
                for g in range(groups) for j in range(5) for c in range(4) if j + c < 7
            ]

        return stage, place, copies

    drains = [value_copy(r, c) for r in range(4) for c in range(8)]
    drains += [stat_copy(d) for d in range(1, NZ)]
    stage, place_of, copies = gatherer(
        gbuf, gsend, grecv, lambda g: g == 0, lambda g: (pl.ds(2 * g, 2),),
        lambda g, c: (2 * g + c,),
    )

    def spread(blocks):
        for g, (j, i) in blocks:
            xx, yy = place_of(g, j, i)
            for r in (2 * g, 2 * g + 1):
                rows = gbuf[xx, yy, r].astype(F32)
                at = pl.ds(pl.multiple_of((4 * (xx * NY + yy) + r) * 24, 8), 16)
                for k in range(4):
                    gf[k, at, :] = rows[:, 128 * k:128 * k + 128]

    def run_gather(stage, use):
        own = [(0, 0)]
        for g in range(2):
            stage(g, 0)
        use([(g, b) for g in range(2) for b in own])
        for n, ready in (
            (1, []), (2, [(1, 0), (2, 0), (0, 1)]), (3, [(0, 2), (3, 0), (1, 1), (1, 2)]),
            (4, [(2, 1), (2, 2), (3, 1), (3, 2)]), (5, [(0, 3)]), (6, [(1, 3), (2, 3)]),
            (7, [(3, 3)]),
        ):
            for g in range(2):
                stage(g, n)
            use([(g, b) for g in range(2) for b in ready])

    for r in range(4):
        combine(r)
    run_gather(stage, spread)
    drains += copies(2)

    big_loads[0].wait()
    swaps[1].wait()

    def head(h, accs):
        lhs = jnp.concatenate(
            [gf[t, pl.ds(h, 64, stride=24), :] for t in range(4)], axis=1
        ).astype(BF)
        return (accs[0] + dot(lhs, wov[0, h], ACROSS), accs[1] + dot(lhs, wov[1, h], ACROSS))

    accs = lax.fori_loop(0, 16, head, (jnp.zeros((64, 224), F32), jnp.zeros((64, 224), F32)), unroll=4)
    for k in range(2):
        es[k] = jnp.concatenate([accs[k], jnp.zeros((64, 32), F32)], axis=1).astype(BF)

    def rows16(q):
        return pl.ds(pl.multiple_of(q * 16, 16), 16)

    def sum_copy(d):
        zz = lax.rem(z + d, NZ)
        return remote(
            es.at[lax.rem(zz, 2), rows16(lax.div(zz, 2))], er.at[z],
            esend.at[d - 1], erecv.at[d - 1], dev(dz=d),
        )

    for d in range(1, NZ):
        sum_copy(d).start()
    drains += [sum_copy(d) for d in range(1, NZ)]
    er[z] = es[zk, rows16(zq)]
    swaps[0].wait()
    hid = jnp.concatenate([hidv[zk].astype(F32), jnp.zeros((32, 128), F32)], axis=0)
    hidt[...] = jnp.transpose(hid)
    hid = hidt[pl.ds(pl.multiple_of(zq * 32, 32), 32), :]
    hid = jnp.concatenate(
        [jnp.where(core == 0, hid[8 * i:8 * i + 4], hid[8 * i + 4:8 * i + 8]) for i in range(4)],
        axis=0,
    )
    for d in range(1, NZ):
        sum_copy(d).wait_recv()
    for b in range(NZ):
        hid = hid + er[b].astype(F32)
    state = hid.astype(BF).astype(F32)
    square = jnp.sum(state * state, axis=1, keepdims=True)
    high = square.astype(BF).astype(F32)
    lanes = lax.broadcasted_iota(jnp.int32, (16, 256), 1)
    state = jnp.where(lanes == 224, high, jnp.where(lanes == 225, square - high, state))
    unit = 2 * zk + lax.div(zq, 2)
    place = pl.ds(pl.multiple_of(16 * lax.rem(zq, 2), 16), 16)
    fg[x, y, unit, place] = state.astype(BF)

    def state_copy(d):
        ref = fg.at[x, y, unit, place]
        return remote(ref, ref, tsend.at[d - 1], trecv.at[d - 1], dev(dz=d))

    for d in range(1, NZ):
        state_copy(d).start()
    for c in drains:
        c.wait_send()
    drains = []
    drains += [state_copy(d) for d in range(1, NZ)]
    for d in range(1, NZ):
        state_copy(d).wait_recv()
    for c in big_loads[1:]:
        c.wait()
    for c in swaps[2:]:
        c.wait()
    stage, place_of, copies = gatherer(
        fg, fsend, frecv, lambda g: g == 0, lambda g: (pl.ds(2 * g, 2),),
        lambda g, c: (2 * g + c,),
    )
    zero = jnp.zeros((64, 256), F32)
    sums = [zero, zero, jnp.zeros((64, 128), F32)]

    def multiply(blocks):
        for g, (j, i) in blocks:
            xx, yy = place_of(g, j, i)
            k = (xx * NY + yy) * 2 + g
            v = fg[xx, yy, pl.ds(2 * g, 2)].reshape(64, 256).astype(F32)
            scale = gainp[pl.ds(8 * lax.rem(k, 4) + lax.div(k, 4), 1), :]
            lhs = (v * scale).astype(BF)
            sums[0] = sums[0] + dot(lhs, wguv[0, k])
            sums[1] = sums[1] + dot(lhs, wguv[1, k])
            sums[2] = sums[2] + v[:, 128:256]

    run_gather(stage, multiply)
    h0, h1, tail = sums
    drains += copies(2)

    norm = lax.rsqrt((tail[:, 96:97] + tail[:, 97:98]) / 7168.0 + EPSILON)
    parts = []
    for k, h in enumerate((h0, h1)):
        gate, up = h[:, :128] * norm, h[:, 128:] * norm
        parts.append(gate / (1.0 + jnp.exp(-gate)) * up * gsel[:, 128 * k:128 * k + 128])
    active = jnp.concatenate(parts, axis=1)
    actf[...] = active
    for i in range(4):
        for j in range(4):
            actp[16 * j + 4 * i:16 * j + 4 * i + 4, :] = actf[16 * i + 4 * j:16 * i + 4 * j + 4, :]
    lhs = (active.astype(BF), actp[...].astype(BF))

    def scatterer(h, along_x, p_ref, m_ref, r_ref, send, recv):
        me = x if along_x else y

        def at(shift):
            return lax.rem(me + shift, 4)

        def copy(c):
            plus = c in (0, 2, 4)
            src, dst = [
                (p_ref.at[h, at(2), :, TOP], m_ref.at[h, 0]),
                (p_ref.at[h, at(2), :, BOT], m_ref.at[h, 1]),
                (p_ref.at[h, at(1), :, BOT], r_ref.at[h, 0, :, BOT]),
                (p_ref.at[h, at(3), :, TOP], r_ref.at[h, 1, :, TOP]),
                (p_ref.at[h, at(1), :, TOP], r_ref.at[h, 0, :, TOP]),
                (p_ref.at[h, at(3), :, BOT], r_ref.at[h, 1, :, BOT]),
            ][c]
            step = 1 if plus else 3
            target = dev(dx=step) if along_x else dev(dy=step)
            return remote(src, dst, send.at[h, c], recv.at[h, c], target)

        def begin():
            for c in range(4):
                copy(c).start()

        def middle():
            for c, shift, part in ((0, 1, TOP), (1, 3, BOT)):
                copy(c).wait_recv()
                joined = p_ref[h, at(shift), :, part].astype(F32) + m_ref[h, c].astype(F32)
                p_ref[h, at(shift), :, part] = joined.astype(p_ref.dtype)
                copy(4 + c).start()

        def end():
            for c in range(2, 6):
                copy(c).wait_recv()
            return (
                p_ref[h, me].astype(F32) + r_ref[h, 0].astype(F32) + r_ref[h, 1].astype(F32)
            )

        return begin, middle, end, [copy(c) for c in range(6)]

    def direct(g, along_x, p_ref, r_ref, send, recv):
        me = x if along_x else y

        def copy(d):
            target = dev(dx=d) if along_x else dev(dy=d)
            src = p_ref.at[g, lax.rem(me + d, 4)]
            return remote(src, r_ref.at[g, d - 1], send.at[g, d - 1], recv.at[g, d - 1], target)

        def begin():
            for d in (2, 1, 3):
                copy(d).start()

        def end():
            total = p_ref[g, me].astype(F32)
            for d in range(1, 4):
                copy(d).wait_recv()
                total = total + r_ref[g, d - 1].astype(F32)
            return total

        return begin, end, [copy(d) for d in range(1, 4)]

    groups = range(4)
    first = [scatterer(g, g % 2 == 0, p1, m1, r1, hsend, hrecv) for g in groups]
    second = [direct(g, g % 2 == 1, p2, r2, ssend, srecv) for g in groups]
    for g in groups:
        base = (g % 2) * HALF + (g // 2) * WIDE
        for c in range(7):
            part = dot(lhs[g % 2], wdv[:, base + 256 * c:base + 256 * c + 256]).astype(BF)
            p1[g, :, :, 256 * c:256 * c + 256] = part.reshape(4, 16, 256)
        first[g][0]()
    for g in groups:
        first[g][1]()
    for g in groups:
        joined = first[g][2]()
        for i in range(4):
            p2[g, i] = joined[4 * i:4 * i + 4].astype(p2.dtype)
        second[g][0]()
    for g in groups:
        joined = second[g][1]()
        for i in range(2):
            z3s[(g % 2) * 4 + (g // 2) * 2 + i] = joined[:, 896 * i:896 * i + 896].astype(z3s.dtype)
        drains += first[g][3] + second[g][2]

    def last_copy(d):
        zz = lax.rem(z + d, NZ)
        return remote(z3s.at[zz], z3r.at[z], zsend.at[d - 1], zrecv.at[d - 1], dev(dz=d))

    for d in range(1, NZ):
        last_copy(d).start()
    drains += [last_copy(d) for d in range(1, NZ)]
    z3r[z] = z3s[z]

    pieces = []
    for i in range(4):
        pe = 2 * z + i // 2
        rows = fg[
            lax.div(pe, 4), lax.rem(pe, 4), 2 * (i % 2) + lax.div(x, 2),
            pl.ds(pl.multiple_of(16 * lax.rem(x, 2), 16), 16),
        ].astype(F32)
        picked = jnp.zeros((4, 256), F32)
        for j in range(4):
            picked = picked + jnp.where(y == j, rows[4 * j:4 * j + 4], 0.0)
        pieces.append(picked[:, :224])
    result = jnp.concatenate(pieces, axis=1)
    for d in range(1, NZ):
        last_copy(d).wait_recv()
    for b in range(NZ):
        result = result + z3r[b].astype(F32)
    out_ref[...] = result
    for c in drains:
        c.wait_send()


def per_device(
    q_latent, q_rope, cache_latent, cache_rope, lengths, w_attn_out, hidden_in, norm_gain,
    w_gate, w_up, w_down, expert_ids, gate_weights,
):
    anywhere = pl.BlockSpec(memory_space=pl.ANY)
    specs = [anywhere] * 13
    specs[4] = pl.BlockSpec(memory_space=pltpu.SMEM)
    vmem = pltpu.VMEM
    dma = pltpu.SemaphoreType.DMA
    scratch = [
        vmem((4, 128, 512), BF), vmem((4, 64, 128), BF), vmem((4, 512, 512), BF),
        vmem((4, 64, 512), BF), vmem((2, 16, 224, 512), BF), vmem((2, 224, 128), BF),
        vmem((56, 128), BF), vmem((2, 32, 256, 256), BF), vmem((256, 7168), BF),
        vmem((8, 128), jnp.int32), vmem((8, 128), F32),
        vmem((4, 128, 512), BF), vmem((8, 128), F32), vmem((8, 8, 128), F32),
        vmem((4, 4, 16, 512), BF), vmem((2, 4, 16, 512), BF), vmem((2, 4, 16, 256), BF),
        vmem((2, 4, 16, 512), BF), vmem((128, 128), F32), vmem((4, 4, 4, 16, 512), BF),
        vmem((4, 1568, 128), F32), vmem((8, 128), F32), vmem((2, 64, 256), BF),
        vmem((8, 16, 256), BF), vmem((4, 4, 4, 32, 256), BF), vmem((128, 256), F32),
        vmem((64, 256), F32), vmem((64, 256), F32), vmem((64, 256), F32),
        vmem((4, 4, 16, WIDE), BF), vmem((4, 2, 16, PART), BF), vmem((4, 2, 16, WIDE), BF),
        vmem((4, 4, 4, WIDE), BF), vmem((4, 3, 4, WIDE), BF),
        vmem((8, 4, 896), BF), vmem((8, 4, 896), BF), vmem((64, 128), F32),
        vmem((32, 256), F32), vmem((128, 256), F32),
        dma((24,)), dma((5,)), dma((5,)), dma((5, 8)), dma((5, 8)),
        dma((2, 5, 4)), dma((2, 5, 4)), dma((7,)), dma((7,)), dma((2, 5, 4)), dma((2, 5, 4)),
        dma((7,)), dma((7,)),
        dma((4, 6)), dma((4, 6)), dma((4, 3)), dma((4, 3)),
        dma((7,)), dma((7,)),
    ]
    return pl.pallas_call(
        kernel,
        out_shape=jax.ShapeDtypeStruct((4, 896), F32),
        in_specs=specs,
        out_specs=pl.BlockSpec(memory_space=pltpu.VMEM),
        scratch_shapes=scratch,
        compiler_params=pltpu.CompilerParams(
            collective_id=0, has_side_effects=True, vmem_limit_bytes=56 * 1024 * 1024
        ),
    )(
        q_latent, q_rope, cache_latent, cache_rope, lengths, jnp.swapaxes(w_attn_out, 1, 2),
        hidden_in.T, norm_gain.reshape(56, 128),
        w_gate.reshape(32, 224, 128), w_up.reshape(32, 224, 128), w_down.reshape(128, 7168),
        expert_ids.T, gate_weights.T,
    ).astype(BF)


def solution(mesh):
    in_specs = (
        P("exp", None, None),
        P("exp", None, None),
        P("exp", "ctx", None),
        P("exp", None, "ctx"),
        P("exp"),
        P("ctx", None, "exp"),
        P(None, "exp"),
        P(),
        P("exp", None, "ctx"),
        P("exp", None, "ctx"),
        P("exp", "ctx", None),
        P(),
        P(),
    )
    return jax.shard_map(
        per_device, mesh=mesh, in_specs=in_specs, out_specs=P("exp", "ctx"), check_vma=False
    )
```

```python
import functools

import jax
import jax.numpy as jnp
from jax import lax
from jax.experimental import pallas as pl
from jax.experimental.pallas import tpu as pltpu
from jax.sharding import PartitionSpec as P

SCALE = 192.0 ** (-0.5)
MASKED = -1e30
EPSILON = 1e-06
MESH = pl.DeviceIdType.MESH
BF = jnp.bfloat16
F32 = jnp.float32
NZ, NX, NY = 8, 4, 4
HALF = 3584
WIDE = 1792
PART = 896
TOP = pl.ds(0, PART)
BOT = pl.ds(PART, PART)
ACROSS = (((1,), (1,)), ((), ()))


def dot(a, b, dims=(((1,), (0,)), ((), ()))):
    return lax.dot_general(a, b, dims, preferred_element_type=F32)


def kernel(
    q_hbm, qr_hbm, kc_hbm, kr_hbm, len_ref, wo_hbm, hid_hbm, gain_hbm, wg_hbm, wu_hbm, wd_hbm,
    ids_hbm, gw_hbm, out_ref,
    qv, qrv, kcv, krv, wov, hidv, gainv, wguv, wdv, idsv, gwv,
    vb, st_s, st_r, br, bm, bh, mg, alv, gbuf, gf, ef, es, er, fg, gds, gsel, actf, actp,
    p1, m1, r1, p2, r2, z3s, z3r, gainf, gainp, hidt,
    lsem, psend, precv, bsend, brecv, gsend, grecv, esend, erecv, fsend, frecv, tsend, trecv,
    hsend, hrecv, ssend, srecv, zsend, zrecv,
):
    z = lax.axis_index("ctx")
    e = lax.axis_index("exp")
    core = lax.rem(e, 2)
    p = lax.div(e, 2)
    y = lax.rem(p, NY)
    x = lax.div(p, NY)
    zq, zk = lax.div(z, 2), lax.rem(z, 2)

    def dev(dz=0, dx=0, dy=0, other=False):
        c = (1 - core) if other else core
        xx, yy = lax.rem(x + dx, NX), lax.rem(y + dy, NY)
        return {"ctx": lax.rem(z + dz, NZ), "exp": (xx * NY + yy) * 2 + c}

    barrier = pltpu.get_barrier_semaphore()
    peers = [dev(dz=d) for d in range(1, NZ)]
    peers += [dev(dx=d) for d in range(1, NX)] + [dev(dy=d) for d in range(1, NY)]
    peers += [dev(other=True)]
    for peer in peers:
        pl.semaphore_signal(barrier, inc=1, device_id=peer, device_id_type=MESH)

    def load(src, dst, k):
        return pltpu.make_async_copy(src, dst, lsem.at[k])

    row_loads = []
    for r in range(4):
        row_loads.append([
            load(q_hbm.at[r], qv.at[r], 4 * r),
            load(kc_hbm.at[r], kcv.at[r], 4 * r + 1),
            load(qr_hbm.at[r], qrv.at[r], 4 * r + 2),
            load(kr_hbm.at[r], krv.at[r], 4 * r + 3),
        ])
        for c in row_loads[r]:
            c.start()
    own = pl.ds(pl.multiple_of(core * 128, 128), 128)
    small_loads = [
        load(ids_hbm, idsv, 16),
        load(gw_hbm, gwv, 17),
        load(gain_hbm, gainv, 18),
        load(hid_hbm, hidv.at[core], 19),
    ]
    big_loads = [
        load(wo_hbm, wov.at[core], 20),
        load(wg_hbm, wguv.at[core, :, pl.ds(0, 224), pl.ds(0, 128)], 21),
        load(wu_hbm, wguv.at[core, :, pl.ds(0, 224), pl.ds(128, 128)], 22),
        load(wd_hbm, wdv.at[own], 23),
    ]
    for c in small_loads + big_loads:
        c.start()
    wguv[:, :, 224:256, :] = jnp.zeros((2, 32, 32, 256), BF)

    pl.semaphore_wait(barrier, len(peers))

    def swap(src, dst, k):
        return pltpu.make_async_remote_copy(
            src_ref=src, dst_ref=dst, send_sem=psend.at[k], recv_sem=precv.at[k],
            device_id=dev(other=True), device_id_type=MESH,
        )

    swaps = [
        swap(hid_hbm, hidv.at[core], 0),
        swap(wo_hbm, wov.at[core], 1),
        swap(wg_hbm, wguv.at[core, :, pl.ds(0, 224), pl.ds(0, 128)], 2),
        swap(wu_hbm, wguv.at[core, :, pl.ds(0, 224), pl.ds(128, 128)], 3),
        swap(wd_hbm, wdv.at[own], 4),
    ]
    for c in swaps:
        c.start()

    def remote(src, dst, ss, rs, device):
        return pltpu.make_async_remote_copy(
            src_ref=src, dst_ref=dst, send_sem=ss, recv_sem=rs,
            device_id=device, device_id_type=MESH,
        )

    def heads_of(zz):
        return pl.ds(pl.multiple_of(zz * 16, 16), 16)

    left256, right256 = pl.ds(0, 256), pl.ds(256, 256)

    def value_copy(r, c):
        src, dst, d = [
            (vb.at[r, heads_of(lax.rem(z + 1, NZ))], br.at[0, r], 1),
            (vb.at[r, heads_of(lax.rem(z + 7, NZ))], br.at[1, r], 7),
            (vb.at[r, heads_of(lax.rem(z + 3, NZ))], bm.at[0, r], 1),
            (vb.at[r, heads_of(lax.rem(z + 5, NZ))], bm.at[1, r], 7),
            (vb.at[r, heads_of(lax.rem(z + 4, NZ)), left256], bh.at[0, r], 2),
            (vb.at[r, heads_of(lax.rem(z + 4, NZ)), right256], bh.at[1, r], 6),
            (mg.at[0, r], br.at[2, r], 2),
            (mg.at[1, r], br.at[3, r], 6),
        ][c]
        return remote(src, dst, bsend.at[r, c], brecv.at[r, c], dev(dz=d))

    def stat_copy(d):
        return remote(st_s, st_r.at[d], bsend.at[4, d], brecv.at[4, d], dev(dz=d))

    lane = lax.broadcasted_iota(jnp.int32, (128, 128), 1)
    position = z * 512 + lax.broadcasted_iota(jnp.int32, (128, 512), 1)
    stats = jnp.zeros((128, 128), F32)
    for r in range(4):
        for c in row_loads[r]:
            c.wait()
        keys = kcv[r]
        scores = dot(qv[r], keys, ACROSS)
        scores = (scores + dot(qrv[r], krv[r], (((0,), (0,)), ((), ())))) * SCALE
        visible = position < len_ref[r]
        scores = jnp.where(visible, scores, MASKED)
        top = jnp.max(scores, axis=1, keepdims=True)
        weights = jnp.where(visible, jnp.exp(scores - top), 0.0)
        total = jnp.sum(weights, axis=1, keepdims=True)
        value = dot(weights.astype(BF), keys)
        held = jnp.maximum(total, 1e-30)
        vb[r] = (value / held).astype(BF)
        lse = jnp.where(total > 0.0, top + jnp.log(held), MASKED)
        stats = jnp.where(lane == r, lse, stats)
        if r == 3:
            st_s[...] = jnp.transpose(stats)[0:8]
            for d in range(1, NZ):
                stat_copy(d).start()
        for c in (2, 3, 4, 5, 0, 1):
            value_copy(r, c).start()
    st_r[0] = st_s[...]

    for c in small_loads:
        c.wait()
    for k in range(2):
        named = jnp.where(idsv[...] == 2 * p + k, gwv[...], 0.0)
        named = jnp.broadcast_to(jnp.sum(named, axis=0, keepdims=True), (128, 128))
        gds[:, 128 * k:128 * k + 128] = jnp.transpose(named)
    gain = gainv[...].astype(F32)
    gainf[0:56, :] = gain
    gain = jnp.concatenate([gainf[pl.ds(t, 8, stride=7), :] for t in range(7)], axis=1)
    for k in range(4):
        gainp[8 * k:8 * k + 8, :] = jnp.concatenate(
            [gain[:, 224 * k:224 * k + 224], jnp.zeros((8, 32), F32)], axis=1
        )
    for i in range(16):
        gsel[4 * i:4 * i + 4, :] = jnp.where(
            core == 0, gds[8 * i:8 * i + 4, :], gds[8 * i + 4:8 * i + 8, :]
        )

    for d in range(1, NZ):
        stat_copy(d).wait_recv()
    s = st_r[...]
    a = jnp.exp(s - jnp.max(s, axis=0, keepdims=True))
    a = a / jnp.sum(a, axis=0, keepdims=True)
    a = jnp.concatenate([a.reshape(64, 128), jnp.zeros((64, 128), F32)], axis=0)
    alv[...] = jnp.transpose(a)
    share = [alv[heads_of(lax.rem(z + d, NZ)), :] for d in (0, 2, 6)]

    def scaled(which, d, r, block):
        return share[which][:, 8 * d + r:8 * d + r + 1] * block.astype(F32)

    for r in range(4):
        for c in (2, 3, 4, 5):
            value_copy(r, c).wait_recv()
        for k, near, far in ((0, 1, 2), (1, 7, 6)):
            to = heads_of(lax.rem(z + (6 if k else 2), NZ))
            joined = scaled(1 + k, 0, r, vb[r, to]) + scaled(1 + k, near, r, bm[k, r])
            half = scaled(1 + k, far, r, bh[k, r])
            pad = jnp.zeros((16, 256), F32)
            joined = joined + jnp.concatenate([half, pad] if k == 0 else [pad, half], axis=1)
            mg[k, r] = joined.astype(BF)
            value_copy(r, 6 + k).start()

    def combine(r):
        for c in (0, 1, 6, 7):
            value_copy(r, c).wait_recv()
        acc = scaled(0, 0, r, vb[r, heads_of(z)])
        acc = acc + scaled(0, 1, r, br[0, r]) + scaled(0, 7, r, br[1, r])
        acc = acc + br[2, r].astype(F32) + br[3, r].astype(F32)
        gbuf[x, y, r] = acc.astype(BF)

    def gatherer(buf, send, recv, x_first, both, forward):
        def region(g, i1, i2, part):
            i1, i2 = lax.rem(i1, 4), lax.rem(i2, 4)
            xx, yy = (i1, i2) if x_first(g) else (i2, i1)
            return buf.at[(xx, yy) + part]

        def copy(g, j, c):
            me1, me2 = (x, y) if x_first(g) else (y, x)
            step = 1 if c in (0, 2) else 3
            part = both(g) if c < 2 else forward(g, c - 2)
            shift = {0: 0, 1: 0, 2: 3, 3: 1}[c]
            if j >= 3 and c == 2:
                step, part, shift = 2, both(g), 0
            if j == 4:
                ref = region(g, me1 + shift, me2, part)
                along_x = x_first(g)
            else:
                column = {0: 0, 1: 3, 2: 1, 3: 2}[j]
                ref = region(g, me1 + column, me2 + shift, part)
                along_x = not x_first(g)
            target = dev(dx=step) if along_x else dev(dy=step)
            return remote(ref, ref, send.at[g, j, c], recv.at[g, j, c], target)

        def place(g, j, i):
            me1, me2 = (x, y) if x_first(g) else (y, x)
            i1 = lax.rem(me1 + {0: 0, 1: 3, 2: 1, 3: 2}[j], 4)
            i2 = lax.rem(me2 + {0: 0, 1: 3, 2: 1, 3: 2}[i], 4)
            return (i1, i2) if x_first(g) else (i2, i1)

        def launch(g, j):
            for c in range(3 if j >= 3 else 2):
                copy(g, j, c).start()

        def pass_on(g, j):
            for c in range(2):
                copy(g, j, c).wait_recv()
                if j == 4:
                    launch(g, 1 + c)
                elif j < 3:
                    copy(g, j, c + 2).start()

        def far(g, j):
            copy(g, j, 2).wait_recv()
            if j == 4:
                launch(g, 3)
            elif j < 3:
                copy(g, j, 3).wait_recv()

        def stage(g, n):
            if n == 0:
                launch(g, 4)
                launch(g, 0)
            elif n == 1:
                pass_on(g, 4)
            elif n == 2:
                pass_on(g, 0)
            elif n == 3:
                far(g, 4)
                pass_on(g, 1)
                pass_on(g, 2)
            elif n == 4:
                pass_on(g, 3)
            elif n == 5:
                far(g, 0)
            elif n == 6:
                far(g, 1)
                far(g, 2)
            else:
                far(g, 3)

        def copies(groups):
            return [
                copy(g, j, c)
                for g in range(groups) for j in range(5) for c in range(4) if j < 3 or c < 3
            ]

        return stage, place, copies

    drains = [value_copy(r, c) for r in range(4) for c in range(8)]
    drains += [stat_copy(d) for d in range(1, NZ)]
    stage, place_of, copies = gatherer(
        gbuf, gsend, grecv, lambda g: g == 0, lambda g: (pl.ds(2 * g, 2),),
        lambda g, c: (2 * g + c,),
    )

    def spread(blocks):
        for g, (j, i) in blocks:
            xx, yy = place_of(g, j, i)
            for r in (2 * g, 2 * g + 1):
                rows = gbuf[xx, yy, r].astype(F32)
                at = pl.ds(pl.multiple_of((4 * (xx * NY + yy) + r) * 24, 8), 16)
                for k in range(4):
                    gf[k, at, :] = rows[:, 128 * k:128 * k + 128]

    def run_gather(stage, use):
        own = [(0, 0)]
        for g in range(2):
            stage(g, 0)
        use([(g, b) for g in range(2) for b in own])
        for n, ready in (
            (1, []), (2, [(1, 0), (2, 0), (0, 1)]), (3, [(0, 2), (3, 0), (1, 1), (1, 2)]),
            (4, [(2, 1), (2, 2), (3, 1), (3, 2)]), (5, [(0, 3)]), (6, [(1, 3), (2, 3)]),
            (7, [(3, 3)]),
        ):
            for g in range(2):
                stage(g, n)
            use([(g, b) for g in range(2) for b in ready])

    for r in range(4):
        combine(r)
    run_gather(stage, spread)
    drains += copies(2)

    big_loads[0].wait()
    swaps[1].wait()

    def head(h, accs):
        lhs = jnp.concatenate(
            [gf[t, pl.ds(h, 64, stride=24), :] for t in range(4)], axis=1
        ).astype(BF)
        return (accs[0] + dot(lhs, wov[0, h], ACROSS), accs[1] + dot(lhs, wov[1, h], ACROSS))

    accs = lax.fori_loop(0, 16, head, (jnp.zeros((64, 224), F32), jnp.zeros((64, 224), F32)), unroll=4)
    for k in range(2):
        es[k] = jnp.concatenate([accs[k], jnp.zeros((64, 32), F32)], axis=1).astype(BF)

    def rows16(q):
        return pl.ds(pl.multiple_of(q * 16, 16), 16)

    def sum_copy(d):
        zz = lax.rem(z + d, NZ)
        return remote(
            es.at[lax.rem(zz, 2), rows16(lax.div(zz, 2))], er.at[z],
            esend.at[d - 1], erecv.at[d - 1], dev(dz=d),
        )

    for d in range(1, NZ):
        sum_copy(d).start()
    drains += [sum_copy(d) for d in range(1, NZ)]
    er[z] = es[zk, rows16(zq)]
    swaps[0].wait()
    hid = jnp.concatenate([hidv[zk].astype(F32), jnp.zeros((32, 128), F32)], axis=0)
    hidt[...] = jnp.transpose(hid)
    hid = hidt[pl.ds(pl.multiple_of(zq * 32, 32), 32), :]
    hid = jnp.concatenate(
        [jnp.where(core == 0, hid[8 * i:8 * i + 4], hid[8 * i + 4:8 * i + 8]) for i in range(4)],
        axis=0,
    )
    for d in range(1, NZ):
        sum_copy(d).wait_recv()
    for b in range(NZ):
        hid = hid + er[b].astype(F32)
    state = hid.astype(BF).astype(F32)
    square = jnp.sum(state * state, axis=1, keepdims=True)
    high = square.astype(BF).astype(F32)
    lanes = lax.broadcasted_iota(jnp.int32, (16, 256), 1)
    state = jnp.where(lanes == 224, high, jnp.where(lanes == 225, square - high, state))
    unit = 2 * zk + lax.div(zq, 2)
    place = pl.ds(pl.multiple_of(16 * lax.rem(zq, 2), 16), 16)
    fg[x, y, unit, place] = state.astype(BF)

    def state_copy(d):
        ref = fg.at[x, y, unit, place]
        return remote(ref, ref, tsend.at[d - 1], trecv.at[d - 1], dev(dz=d))

    for d in range(1, NZ):
        state_copy(d).start()
    for c in drains:
        c.wait_send()
    drains = []
    drains += [state_copy(d) for d in range(1, NZ)]
    for d in range(1, NZ):
        state_copy(d).wait_recv()
    for c in big_loads[1:]:
        c.wait()
    for c in swaps[2:]:
        c.wait()
    stage, place_of, copies = gatherer(
        fg, fsend, frecv, lambda g: g == 0, lambda g: (pl.ds(2 * g, 2),),
        lambda g, c: (2 * g + c,),
    )
    zero = jnp.zeros((64, 256), F32)
    sums = [zero, zero, jnp.zeros((64, 128), F32)]

    def multiply(blocks):
        for g, (j, i) in blocks:
            xx, yy = place_of(g, j, i)
            k = (xx * NY + yy) * 2 + g
            v = fg[xx, yy, pl.ds(2 * g, 2)].reshape(64, 256).astype(F32)
            scale = gainp[pl.ds(8 * lax.rem(k, 4) + lax.div(k, 4), 1), :]
            lhs = (v * scale).astype(BF)
            sums[0] = sums[0] + dot(lhs, wguv[0, k])
            sums[1] = sums[1] + dot(lhs, wguv[1, k])
            sums[2] = sums[2] + v[:, 128:256]

    run_gather(stage, multiply)
    h0, h1, tail = sums
    drains += copies(2)

    norm = lax.rsqrt((tail[:, 96:97] + tail[:, 97:98]) / 7168.0 + EPSILON)
    parts = []
    for k, h in enumerate((h0, h1)):
        gate, up = h[:, :128] * norm, h[:, 128:] * norm
        parts.append(gate / (1.0 + jnp.exp(-gate)) * up * gsel[:, 128 * k:128 * k + 128])
    active = jnp.concatenate(parts, axis=1)
    actf[...] = active
    for i in range(4):
        for j in range(4):
            actp[16 * j + 4 * i:16 * j + 4 * i + 4, :] = actf[16 * i + 4 * j:16 * i + 4 * j + 4, :]
    lhs = (active.astype(BF), actp[...].astype(BF))

    def scatterer(h, along_x, p_ref, m_ref, r_ref, send, recv):
        me = x if along_x else y

        def at(shift):
            return lax.rem(me + shift, 4)

        def copy(c):
            plus = c in (0, 2, 4)
            src, dst = [
                (p_ref.at[h, at(2), :, TOP], m_ref.at[h, 0]),
                (p_ref.at[h, at(2), :, BOT], m_ref.at[h, 1]),
                (p_ref.at[h, at(1), :, BOT], r_ref.at[h, 0, :, BOT]),
                (p_ref.at[h, at(3), :, TOP], r_ref.at[h, 1, :, TOP]),
                (p_ref.at[h, at(1), :, TOP], r_ref.at[h, 0, :, TOP]),
                (p_ref.at[h, at(3), :, BOT], r_ref.at[h, 1, :, BOT]),
            ][c]
            step = 1 if plus else 3
            target = dev(dx=step) if along_x else dev(dy=step)
            return remote(src, dst, send.at[h, c], recv.at[h, c], target)

        def begin():
            for c in range(4):
                copy(c).start()

        def middle():
            for c, shift, part in ((0, 1, TOP), (1, 3, BOT)):
                copy(c).wait_recv()
                joined = p_ref[h, at(shift), :, part].astype(F32) + m_ref[h, c].astype(F32)
                p_ref[h, at(shift), :, part] = joined.astype(p_ref.dtype)
                copy(4 + c).start()

        def end():
            for c in range(2, 6):
                copy(c).wait_recv()
            return (
                p_ref[h, me].astype(F32) + r_ref[h, 0].astype(F32) + r_ref[h, 1].astype(F32)
            )

        return begin, middle, end, [copy(c) for c in range(6)]

    def direct(g, along_x, p_ref, r_ref, send, recv):
        me = x if along_x else y

        def copy(d):
            target = dev(dx=d) if along_x else dev(dy=d)
            src = p_ref.at[g, lax.rem(me + d, 4)]
            return remote(src, r_ref.at[g, d - 1], send.at[g, d - 1], recv.at[g, d - 1], target)

        def begin():
            for d in (2, 1, 3):
                copy(d).start()

        def end():
            total = p_ref[g, me].astype(F32)
            for d in range(1, 4):
                copy(d).wait_recv()
                total = total + r_ref[g, d - 1].astype(F32)
            return total

        return begin, end, [copy(d) for d in range(1, 4)]

    groups = range(4)
    first = [scatterer(g, g % 2 == 0, p1, m1, r1, hsend, hrecv) for g in groups]
    second = [direct(g, g % 2 == 1, p2, r2, ssend, srecv) for g in groups]
    for g in groups:
        base = (g % 2) * HALF + (g // 2) * WIDE
        for c in range(7):
            part = dot(lhs[g % 2], wdv[:, base + 256 * c:base + 256 * c + 256]).astype(BF)
            p1[g, :, :, 256 * c:256 * c + 256] = part.reshape(4, 16, 256)
        first[g][0]()
    for g in groups:
        first[g][1]()
    for g in groups:
        joined = first[g][2]()
        for i in range(4):
            p2[g, i] = joined[4 * i:4 * i + 4].astype(p2.dtype)
        second[g][0]()
    for g in groups:
        joined = second[g][1]()
        for i in range(2):
            z3s[(g % 2) * 4 + (g // 2) * 2 + i] = joined[:, 896 * i:896 * i + 896].astype(z3s.dtype)
        drains += first[g][3] + second[g][2]

    def last_copy(d):
        zz = lax.rem(z + d, NZ)
        return remote(z3s.at[zz], z3r.at[z], zsend.at[d - 1], zrecv.at[d - 1], dev(dz=d))

    for d in range(1, NZ):
        last_copy(d).start()
    drains += [last_copy(d) for d in range(1, NZ)]
    z3r[z] = z3s[z]

    pieces = []
    for i in range(4):
        pe = 2 * z + i // 2
        rows = fg[
            lax.div(pe, 4), lax.rem(pe, 4), 2 * (i % 2) + lax.div(x, 2),
            pl.ds(pl.multiple_of(16 * lax.rem(x, 2), 16), 16),
        ].astype(F32)
        picked = jnp.zeros((4, 256), F32)
        for j in range(4):
            picked = picked + jnp.where(y == j, rows[4 * j:4 * j + 4], 0.0)
        pieces.append(picked[:, :224])
    result = jnp.concatenate(pieces, axis=1)
    for d in range(1, NZ):
        last_copy(d).wait_recv()
    for b in range(NZ):
        result = result + z3r[b].astype(F32)
    out_ref[...] = result
    for c in drains:
        c.wait_send()


def per_device(
    q_latent, q_rope, cache_latent, cache_rope, lengths, w_attn_out, hidden_in, norm_gain,
    w_gate, w_up, w_down, expert_ids, gate_weights,
):
    anywhere = pl.BlockSpec(memory_space=pl.ANY)
    specs = [anywhere] * 13
    specs[4] = pl.BlockSpec(memory_space=pltpu.SMEM)
    vmem = pltpu.VMEM
    dma = pltpu.SemaphoreType.DMA
    scratch = [
        vmem((4, 128, 512), BF), vmem((4, 64, 128), BF), vmem((4, 512, 512), BF),
        vmem((4, 64, 512), BF), vmem((2, 16, 224, 512), BF), vmem((2, 224, 128), BF),
        vmem((56, 128), BF), vmem((2, 32, 256, 256), BF), vmem((256, 7168), BF),
        vmem((8, 128), jnp.int32), vmem((8, 128), F32),
        vmem((4, 128, 512), BF), vmem((8, 128), F32), vmem((8, 8, 128), F32),
        vmem((4, 4, 16, 512), BF), vmem((2, 4, 16, 512), BF), vmem((2, 4, 16, 256), BF),
        vmem((2, 4, 16, 512), BF), vmem((128, 128), F32), vmem((4, 4, 4, 16, 512), BF),
        vmem((4, 1568, 128), F32), vmem((8, 128), F32), vmem((2, 64, 256), BF),
        vmem((8, 16, 256), BF), vmem((4, 4, 4, 32, 256), BF), vmem((128, 256), F32),
        vmem((64, 256), F32), vmem((64, 256), F32), vmem((64, 256), F32),
        vmem((4, 4, 16, WIDE), BF), vmem((4, 2, 16, PART), BF), vmem((4, 2, 16, WIDE), BF),
        vmem((4, 4, 4, WIDE), BF), vmem((4, 3, 4, WIDE), BF),
        vmem((8, 4, 896), BF), vmem((8, 4, 896), BF), vmem((64, 128), F32),
        vmem((32, 256), F32), vmem((128, 256), F32),
        dma((24,)), dma((5,)), dma((5,)), dma((5, 8)), dma((5, 8)),
        dma((2, 5, 4)), dma((2, 5, 4)), dma((7,)), dma((7,)), dma((2, 5, 4)), dma((2, 5, 4)),
        dma((7,)), dma((7,)),
        dma((4, 6)), dma((4, 6)), dma((4, 3)), dma((4, 3)),
        dma((7,)), dma((7,)),
    ]
    return pl.pallas_call(
        kernel,
        out_shape=jax.ShapeDtypeStruct((4, 896), F32),
        in_specs=specs,
        out_specs=pl.BlockSpec(memory_space=pltpu.VMEM),
        scratch_shapes=scratch,
        compiler_params=pltpu.CompilerParams(
            collective_id=0, has_side_effects=True, vmem_limit_bytes=56 * 1024 * 1024
        ),
    )(
        q_latent, q_rope, cache_latent, cache_rope, lengths, jnp.swapaxes(w_attn_out, 1, 2),
        hidden_in.T, norm_gain.reshape(56, 128),
        w_gate.reshape(32, 224, 128), w_up.reshape(32, 224, 128), w_down.reshape(128, 7168),
        expert_ids.T, gate_weights.T,
    ).astype(BF)


def solution(mesh):
    in_specs = (
        P("exp", None, None),
        P("exp", None, None),
        P("exp", "ctx", None),
        P("exp", None, "ctx"),
        P("exp"),
        P("ctx", None, "exp"),
        P(None, "exp"),
        P(),
        P("exp", None, "ctx"),
        P("exp", None, "ctx"),
        P("exp", "ctx", None),
        P(),
        P(),
    )
    return jax.shard_map(
        per_device, mesh=mesh, in_specs=in_specs, out_specs=P("exp", "ctx"), check_vma=False
    )
```
